32 devices in a mesh: dp: 8 (over z, x), mp: 4 (over y, core).
Axes of the slice: x: 2, y: 2, z: 4, core: 2. Of those that a mesh axis runs over, the one named last changes fastest.
Arguments:
- query_rows: bfloat16 [512, 2560], P('dp', 'mp'), may hold values from -48 to 48
- doc_rows: bfloat16 [512, 2560], P('dp', 'mp'), may hold values from -48 to 48
- head: bfloat16 [2560, 2560], P(None, 'mp'), may hold values from -0.125 to 0.125
- logit_scale: float32 [7], replicated, may hold values from 1 to 3
- loss_grad: float32 [512, 7], P('dp'), may hold values from 0.5 to 2
- shortlist: int32 [512, 128], P('dp'), may hold values from 0 to 127, as said below
- send_rows: int32 [8, 128], P('dp'), may hold values from -1 to 63, as said below
Outputs:
- query_grad: bfloat16 [512, 2560], P('dp', 'mp')
- doc_grad: bfloat16 [512, 2560], P('dp', 'mp')
- head_grad: float32 [2560, 2560], P('dp', 'mp')
The draws below stay inside these ranges and needn't reach their ends.
Inputs may be any that keep to these rules, and one draw needn't show every extreme that they name: shortlist[i, n] is a slot o * 16 + j of the rows fetched for the owner of query i, and send_rows at place j of the block owner o sends to that owner is never -1. send_rows[o, r * 16 + j] is a row among owner o's 64 documents, sent to owner r at place j; in each block of 16 places the rows are distinct and come first, -1 fills the rest; the block an owner sends to itself is always full.
All inputs are finite; a program needn't handle non-finite values.
Results may differ from the reference program's by a relative error of at most 0.014.
The reference program's roundings to bfloat16 on the way count: a program that leaves them out, or rounds other values in their place, can miss the bound.
Values may be sent and summed in bfloat16 or wider, within the bound.
A program may use at most 64 MiB of HBM per device.

```python
import math
import jax
import jax.numpy as jnp
from jax import lax

D = 2560
QL = 64
NEG = 128
NW = 7
NQ = 512
FETCH_ROWS = 128
N_DP = 8


def fetch_plan(key):
    fetch_block = FETCH_ROWS // N_DP
    base_key = jax.random.fold_in(key, 7001)
    count_key, order_key, owner_key, pick_key = jax.random.split(base_key, 4)
    least_count = (fetch_block + 1) // 2
    counts = jax.random.randint(count_key, (N_DP, N_DP), least_count, fetch_block + 1)
    diagonal = jnp.arange(N_DP)[:, None] == jnp.arange(N_DP)[None, :]
    counts = jnp.where(diagonal, fetch_block, counts)
    ranking = jax.random.randint(order_key, (N_DP, N_DP, QL), 0, 1 << 20) * QL + jnp.arange(QL)[None, None, :]
    row_order = jnp.argsort(ranking, axis=2)[:, :, :fetch_block]
    place_ids = jnp.arange(fetch_block)[None, None, :]
    sent_rows = jnp.where(place_ids < counts[:, :, None], row_order, -1).astype(jnp.int32)
    send_rows = sent_rows.reshape(N_DP, N_DP * fetch_block)
    owners = jax.random.randint(owner_key, (NQ, NEG), 0, N_DP)
    requester = jnp.broadcast_to((jnp.arange(NQ) // QL)[:, None], (NQ, NEG))
    available = counts[owners, requester]
    place_pick = jax.random.randint(pick_key, (NQ, NEG), 0, 1 << 16) % available
    shortlist = (owners * fetch_block + place_pick).astype(jnp.int32)
    return (send_rows, shortlist)


def embed_pair(key):
    base_key = jax.random.fold_in(key, 7002)
    query_key, doc_key = jax.random.split(base_key, 2)
    query_vals = jax.random.normal(query_key, (NQ, D), jnp.float32)
    doc_vals = jax.random.normal(doc_key, (NQ, D), jnp.float32)
    return (query_vals, doc_vals)


def draw_query_rows(key, part):
    return embed_pair(key)[0].astype(jnp.bfloat16)


def draw_doc_rows(key, part):
    return embed_pair(key)[1].astype(jnp.bfloat16)


def draw_shortlist(key, part):
    return fetch_plan(key)[1]


def draw_send_rows(key, part):
    return fetch_plan(key)[0]


def block_levels(own_key, shape, cuts, least, high):
    def one(position, blocks):
        draws = jax.random.uniform(jax.random.fold_in(jax.random.fold_in(own_key, 6), position), (blocks,), jnp.float32, least / len(cuts), high / len(cuts))
        return jnp.repeat(jnp.exp(draws), shape[position] // blocks).reshape((-1,) + (1,) * (len(shape) - position - 1))

    level = one(*cuts[0])
    for cut in cuts[1:]:
        level = level * one(*cut)
    return level


def bell_draw(rng, extent, width, limit, cuts=(), kind=jnp.bfloat16):
    values = width * jax.random.normal(rng, extent, jnp.float32)
    if cuts:
        values = values * block_levels(rng, extent, cuts, -0.22, 0.18)
    return jnp.clip(values, -limit, limit).astype(kind)


def setup_inputs(seed: int = 0) -> dict:
    streams_of = jax.random.split(jax.random.key(seed), 8)
    return {
        "query_rows": draw_query_rows(jax.random.fold_in(streams_of[7], 71), 0),
        "doc_rows": draw_doc_rows(jax.random.fold_in(streams_of[7], 71), 0),
        "head": bell_draw(streams_of[2], (D, D), D ** -0.5, 0.125, ((1, 4),)),
        "logit_scale": jnp.clip(jnp.exp(jax.random.uniform(streams_of[3], (NW,), jnp.float32, math.log(1.0), math.log(3.0))), 1.0, 3.0),
        "loss_grad": jnp.clip(jnp.exp(math.log(2.0) - 1.3862944 * jax.random.uniform(streams_of[4], (NQ, NW), jnp.float32) ** block_levels(streams_of[4], (NQ, NW), ((0, 8),), -0.2, 0.2)), 0.5, 2.0),
        "shortlist": draw_shortlist(jax.random.fold_in(streams_of[7], 71), 0),
        "send_rows": draw_send_rows(jax.random.fold_in(streams_of[7], 71), 0),
    }


def width_bounds():
    return [0] + [D // 2 ** (NW - 1 - width_level) for width_level in range(NW)]

def softmax_terms(neg_score, pos_score, width_scale, loss_weight):
    neg_logit = neg_score * width_scale[:, None, None]
    pos_logit = pos_score * width_scale[:, None]
    highest = jnp.maximum(lax.optimization_barrier(jnp.max(neg_logit, axis=2)), pos_logit)
    neg_exp = jnp.exp(neg_logit - highest[:, :, None])
    pos_exp = jnp.exp(pos_logit - highest)
    denominator = lax.optimization_barrier(jnp.sum(neg_exp, axis=2)) + pos_exp
    row_weight = loss_weight * width_scale[:, None]
    neg_grad = neg_exp * (row_weight / denominator)[:, :, None]
    pos_grad = row_weight * (pos_exp / denominator - 1.0)
    return (neg_grad, pos_grad)

def suffix_sum(values):
    return jnp.flip(jnp.cumsum(jnp.flip(values, 0), axis=0), 0)

def reference(query_rows, doc_rows, head, logit_scale, loss_grad, shortlist, send_rows):
    bounds = width_bounds()
    fetch_block = FETCH_ROWS // N_DP
    query_proj = jnp.dot(query_rows, head, preferred_element_type=jnp.float32).astype(jnp.bfloat16)
    doc_proj = jnp.dot(doc_rows, head, preferred_element_type=jnp.float32).astype(jnp.bfloat16)
    widths = jnp.array(bounds[1:], jnp.float32)
    width_scale = logit_scale / jnp.sqrt(widths)
    slot_ids = jnp.arange(FETCH_ROWS, dtype=jnp.int32)
    slot_owner = slot_ids // fetch_block
    slot_place = slot_ids % fetch_block
    col_ids = jnp.arange(D, dtype=jnp.int32)
    seg_onehot = jnp.stack([((col_ids >= bounds[segment]) & (col_ids < bounds[segment + 1])).astype(jnp.float32) for segment in range(NW)])
    query_ids = jnp.arange(QL, dtype=jnp.int32)

    def one_owner(doc_accum, inputs):
        owner_index, owner_query, owner_doc, shortlisted, weight_rows = inputs
        local_rows = send_rows[slot_owner, owner_index * fetch_block + slot_place]
        is_valid = local_rows >= 0
        doc_ids = (slot_owner * QL + jnp.maximum(local_rows, 0)).astype(jnp.int32)
        fetched = doc_proj[doc_ids]
        pieces = []
        for segment in range(NW):
            lower, upper = (bounds[segment], bounds[segment + 1])
            pieces.append(jnp.dot(owner_query[:, lower:upper], fetched[:, lower:upper].T, preferred_element_type=jnp.float32))
        scores = jnp.cumsum(jnp.stack(pieces), axis=0)
        neg_score = jnp.take_along_axis(scores, jnp.broadcast_to(shortlisted[None], (NW, QL, NEG)), axis=2)
        pos_prod = owner_query.astype(jnp.float32) * owner_doc.astype(jnp.float32)
        pos_score = jnp.cumsum(jnp.dot(seg_onehot, pos_prod.T, precision=lax.Precision.HIGHEST), axis=0)
        neg_grad, pos_grad = softmax_terms(neg_score, pos_score, width_scale, weight_rows.T)
        seg_neg = suffix_sum(neg_grad)
        seg_pos = suffix_sum(pos_grad)
        coeff_dense = jax.vmap(lambda values: jnp.zeros((QL, FETCH_ROWS), jnp.float32).at[query_ids[:, None], shortlisted].add(values))(seg_neg).astype(jnp.bfloat16)
        pos_cols = jnp.dot(seg_pos.T, seg_onehot, precision=lax.Precision.HIGHEST)
        query_parts = []
        fetched_parts = []
        for segment in range(NW):
            lower, upper = (bounds[segment], bounds[segment + 1])
            query_parts.append(jnp.dot(coeff_dense[segment], fetched[:, lower:upper], preferred_element_type=jnp.float32))
            fetched_parts.append(jnp.dot(coeff_dense[segment].T, owner_query[:, lower:upper], preferred_element_type=jnp.float32))
        query_back = jnp.concatenate(query_parts, axis=1) + pos_cols * owner_doc.astype(jnp.float32)
        fetched_grad = jnp.concatenate(fetched_parts, axis=1)
        targets = jnp.where(is_valid, doc_ids, NQ).astype(jnp.int32)
        doc_accum = doc_accum.at[targets].add(fetched_grad, mode='drop')
        own_start = (owner_index * QL).astype(jnp.int32)
        own_rows = lax.dynamic_slice_in_dim(doc_accum, own_start, QL, 0) + pos_cols * owner_query.astype(jnp.float32)
        doc_accum = lax.dynamic_update_slice_in_dim(doc_accum, own_rows, own_start, 0)
        return (doc_accum, query_back.astype(jnp.bfloat16))
    owner_range = jnp.arange(N_DP, dtype=jnp.int32)
    inputs = (owner_range, query_proj.reshape(N_DP, QL, D), doc_proj.reshape(N_DP, QL, D), shortlist.reshape(N_DP, QL, NEG), loss_grad.reshape(N_DP, QL, NW))
    doc_accum, query_back = lax.scan(one_owner, jnp.zeros((NQ, D), jnp.float32), inputs)
    grad_proj_q = query_back.reshape(NQ, D)
    grad_proj_d = doc_accum.astype(jnp.bfloat16)
    query_grad = jnp.dot(grad_proj_q, head.T, preferred_element_type=jnp.float32).astype(jnp.bfloat16)
    doc_grad = jnp.dot(grad_proj_d, head.T, preferred_element_type=jnp.float32).astype(jnp.bfloat16)
    head_grad = jnp.dot(query_rows.T, grad_proj_q, preferred_element_type=jnp.float32) + jnp.dot(doc_rows.T, grad_proj_d, preferred_element_type=jnp.float32)
    return (query_grad, doc_grad, head_grad)
```

```python
import functools
import math

import jax
import jax.numpy as jnp
from jax import lax
from jax.experimental import pallas as pl
from jax.experimental.pallas import tpu as pltpu
from jax.sharding import PartitionSpec as P

NW = 7
PARTS = 2
MESH = pl.DeviceIdType.MESH
BF = jnp.bfloat16
F32 = jnp.float32


def width_bounds(feature_total):
    return [0] + [feature_total // 2 ** (NW - 1 - level) for level in range(NW)]


def local_segments(bounds, cols):
    return sum(bound <= cols for bound in bounds[1:])


def flip_bits(value, mask):
    bit = 1
    while bit <= mask:
        if mask & bit:
            value = value + bit - 2 * bit * lax.rem(lax.div(value, bit), 2)
        bit *= 2
    return value


def kernel(
    n_dp,
    n_mp,
    q_hbm,
    d_hbm,
    head_hbm,
    scale_hbm,
    weight_hbm,
    short_hbm,
    rows_hbm,
    qg_ref,
    dg_ref,
    hg_ref,
    q_ref,
    d_ref,
    scale_ref,
    weight_ref,
    short_ref,
    rows_ref,
    head,
    whole,
    own_t,
    rows_t,
    f_out,
    f_in,
    ex_out,
    ex_in,
    coef,
    r_out,
    r_in,
    grads,
    part_out,
    part_in,
    flat,
    ssem,
    rsem,
    lsem,
):
    ql, cols = q_ref.shape
    total = n_mp * cols
    slots = rows_ref.shape[1]
    blk = slots // n_dp
    chunk = total // n_dp
    per_mp = n_dp // n_mp
    half = n_dp // 2
    bounds = width_bounds(total)
    n_loc = local_segments(bounds, cols)
    r = lax.axis_index("dp")
    m = lax.axis_index("mp")
    partner = flip_bits(r, 1)

    counts = {}

    def alloc(kind, n):
        start = counts.get(kind, 0)
        counts[kind] = start + n
        return start

    def remote(src, dst, s, t, **where):
        return pltpu.make_async_remote_copy(
            src_ref=src,
            dst_ref=dst,
            send_sem=ssem.at[s],
            recv_sem=rsem.at[t],
            device_id=where,
            device_id_type=MESH,
        )

    loads = [
        pltpu.make_async_copy(src, dst, lsem.at[2 + i])
        for i, (src, dst) in enumerate(
            [
                (d_hbm, d_ref),
                (q_hbm, q_ref),
                (rows_hbm, rows_ref),
                (short_hbm, short_ref),
                (weight_hbm, weight_ref),
                (scale_hbm, scale_ref),
            ]
        )
    ]
    for copy in loads:
        copy.start()
    head_copy = pltpu.make_async_copy(head_hbm, head, lsem.at[0])
    head_copy.start()
    barrier = pltpu.get_barrier_semaphore()
    for j in range(1, n_mp):
        pl.semaphore_signal(
            barrier, inc=1, device_id={"mp": flip_bits(m, j)}, device_id_type=MESH
        )
    for k in range(1, n_dp):
        pl.semaphore_signal(
            barrier, inc=1, device_id={"dp": lax.rem(r + k, n_dp)}, device_id_type=MESH
        )
    for copy in loads:
        copy.wait()
    pl.semaphore_wait(barrier, n_mp - 1 + n_dp - 1)

    sent = []
    parts = PARTS

    s0 = alloc("s", 2 * (n_mp - 1))
    t0 = alloc("r", 2 * (n_mp - 1))
    row_copies = []
    for h, ref in enumerate((d_ref, q_ref)):
        base = h * (n_mp - 1) - 1
        copies = {}
        for j in [*range(2, n_mp, 2), 1]:
            copies[j] = remote(
                ref, whole.at[m, h], s0 + base + j, t0 + base + j, mp=flip_bits(m, j)
            )
            copies[j].start()
        for j in range(2, n_mp, 2):
            k = flip_bits(m, j)
            copies[j + 1] = remote(
                whole.at[k, h],
                whole.at[k, h],
                s0 + base + j + 1,
                t0 + base + j + 1,
                mp=flip_bits(m, 1),
            )
        row_copies.append(copies)
        sent.extend(copies.values())

    def exchange(out, into):
        s = alloc("s", n_dp - 1)
        t = alloc("r", n_dp - 1)
        copies = []
        for k in range(1, n_dp):
            peer = lax.rem(r + k, n_dp)
            copy = remote(out(peer), into(peer), s + k - 1, t + k - 1, dp=peer)
            copy.start()
            copies.append(copy)
            sent.append(copy)
        return copies

    own = jnp.concatenate([d_ref[...], q_ref[...]], axis=0)
    own_t[...] = jnp.transpose(own)
    s_t = alloc("s", per_mp)
    t_t = alloc("r", n_dp)
    place = lax.div(r, 2)
    side = lax.rem(r, 2)
    keeper = lax.div(r, per_mp)

    def spread(late, step):
        for i in range(per_mp // 2):
            c = 2 * i + (1 - side if late else side)
            target = m * per_mp + c
            copy = remote(
                own_t.at[pl.ds(pl.multiple_of(c * chunk, 16), chunk)],
                rows_t.at[side, place],
                s_t + 2 * i + int(late),
                t_t + r,
                dp=target,
            )
            if late:
                step(copy)
            else:
                pl.when(target != r)(functools.partial(step, copy))

    spread(False, lambda copy: copy.start())

    @pl.when(m == keeper)
    def _():
        c = lax.rem(r, per_mp)
        rows_t[side, place] = own_t[pl.ds(pl.multiple_of(c * chunk, 16), chunk), :]

    s_f = alloc("s", 2 * (n_mp - 1))
    t_f = alloc("r", 2)
    same = lax.rem(m, 2) == lax.rem(keeper, 2)
    passes = jnp.logical_and(same, m != keeper)

    def hand_over(late):
        ref = rows_t.at[1 - side if late else side]
        first = s_f + int(late) * (n_mp - 1) - 1
        return [
            remote(ref, ref, first + j, t_f + int(late), mp=flip_bits(m, j))
            for j in [*range(2, n_mp, 2), 1]
        ]

    halves = [hand_over(False), hand_over(True)]

    def hand_start(late):
        @pl.when(m == keeper)
        def _():
            for p in range(half):
                origin = 2 * p + (1 - side if late else side)

                @pl.when(r != origin)
                def _(p=p, origin=origin):
                    remote(
                        own_t.at[pl.ds(0, chunk)],
                        rows_t.at[1 - side if late else side, p],
                        s_t,
                        t_t + origin,
                        dp=r,
                    ).wait_recv()

            for copy in halves[late]:
                copy.start()

    def hand_pass(late):
        @pl.when(passes)
        def _():
            halves[late][-1].wait_recv()
            halves[late][-1].start()

    def hand_end(late):
        @pl.when(jnp.logical_not(same))
        def _():
            halves[late][-1].wait_recv()

    head_copy.wait()

    def head_rows(k):
        return head[pl.ds(pl.multiple_of(k * cols, cols), cols), :]

    def project(h, ref):
        copies = row_copies[h]
        acc = jnp.dot(ref[...], head_rows(m), preferred_element_type=F32)
        for j in range(1, n_mp, 2):
            for i in [j] if j == 1 else [j - 1, j]:
                k = flip_bits(m, i)
                copies[i].wait_recv()
                if i % 2 == 0:
                    copies[i + 1].start()
                acc = acc + jnp.dot(whole[k, h], head_rows(k), preferred_element_type=F32)
        return acc.astype(BF)

    class Gather:
        def __init__(self, piece, parts):
            self.piece = piece
            self.parts = parts
            self.s = alloc("s", parts * (4 * half - 1))
            self.t = alloc("r", parts * 2 * half)
            self.used = 0
            self.own = [
                ([self.copy(r, c, dz) for c in range(parts)], self.within(dz))
                for dz in (-1, 1)
            ]
            self.across = [self.copy(r, c, 0) for c in range(parts)]
            self.hops = {}
            for d in range(1, half):
                self.hops[d] = []
                for dz in (-1, 1):
                    origin = lax.rem(r - 2 * dz * d + 2 * n_dp, n_dp)
                    steps = [
                        (self.copy(origin, c, dz), self.copy(origin, c, 0))
                        for c in range(parts)
                    ]
                    self.hops[d].append((origin, self.within(-dz * d), self.within(dz), steps))

        def within(self, step):
            return place + step >= 0 if step < 0 else place + step < half

        def copy(self, origin, c, dz):
            ref = self.piece(origin, c)
            row = lax.div(origin, 2) + (half if dz == 0 else 0)
            target = lax.rem(r + 2 * dz + n_dp, n_dp) if dz else partner
            self.used += 1
            return remote(
                ref, ref, self.s + self.used - 1, self.t + row * self.parts + c, dp=target
            )

        def start(self):
            for copies, inside in self.own:

                @pl.when(inside)
                def _(copies=copies):
                    for copy in copies:
                        copy.start()

            for copy in self.across:
                copy.start()

        def forward(self, *hops):
            for d in hops:
                for origin, there, further, steps in self.hops[d]:

                    @pl.when(there)
                    def _(further=further, steps=steps):
                        for relay, over in steps:
                            relay.wait_recv()
                            pl.when(further)(relay.start)
                            over.start()

        def finish(self, line):
            for c in range(self.parts):
                self.copy_from_partner(line, c).wait_recv()

        def copy_from_partner(self, line, c):
            ref = self.piece(line * 2 + 1 - side, c)
            row = self.t + (line + half) * self.parts + c
            return remote(ref, ref, self.s, row, dp=partner)

        def drain(self):
            for copies, inside in self.own:

                @pl.when(inside)
                def _(copies=copies):
                    for copy in copies:
                        copy.wait_send()

            for copy in self.across:
                copy.wait_send()
            for hops in self.hops.values():
                for origin, there, further, steps in hops:

                    @pl.when(there)
                    def _(further=further, steps=steps):
                        for _, over in steps:
                            over.wait_send()

                        @pl.when(further)
                        def _():
                            for relay, _ in steps:
                                relay.wait_send()

    slot_ids = lax.broadcasted_iota(jnp.int32, (ql, slots), 1)
    row_ids = lax.broadcasted_iota(jnp.int32, (ql, slots), 0)
    eye = slot_ids == row_ids
    from_rows = (((0,), (0,)), ((), ()))

    sel_t32 = jnp.where(rows_ref[...] == row_ids, 1.0, 0.0)
    sel_t = sel_t32.astype(BF)
    sel = jnp.transpose(sel_t32).astype(BF)
    doc = project(0, d_ref)

    def to_blocks(values, out):
        if blk % 16 == 0:
            out[...] = values.astype(BF).reshape(n_dp, blk, cols)
        else:
            flat[...] = values
            for p in range(n_dp):
                out[p] = flat[p * blk : (p + 1) * blk, :].astype(BF)

    def from_blocks(buf):
        if blk % 16 == 0:
            return buf[...].reshape(slots, cols)
        for p in range(n_dp):
            flat[p * blk : (p + 1) * blk, :] = buf[p].astype(F32)
        return flat[...].astype(BF)

    to_blocks(jnp.dot(sel, doc, preferred_element_type=F32), f_out)
    fetches = exchange(lambda peer: f_out.at[peer], lambda peer: f_in.at[r])
    f_in[r] = f_out[r]
    query = project(1, q_ref)
    hand_start(0)

    short = short_ref[...]
    named = jnp.zeros((ql, slots), F32)
    for n in range(short.shape[1]):
        named = named + jnp.where(short[:, n : n + 1] == slot_ids, 1.0, 0.0)

    col_ids = lax.broadcasted_iota(jnp.int32, (1, cols), 1)
    seg = [
        jnp.where(jnp.logical_and(col_ids >= bounds[s], col_ids < bounds[s + 1]), 1.0, 0.0)
        for s in range(n_loc)
    ]
    cut = min(256, cols)
    groups = [
        (lo, hi, [s for s in range(n_loc) if bounds[s] < hi and bounds[s + 1] > lo])
        for lo, hi in ((0, cut), (cut, cols))
        if lo < hi
    ]
    below = [jnp.where(col_ids < bounds[w + 1], 1.0, 0.0) for w in range(n_loc - 1)]
    q_prefix = jnp.concatenate([query * b.astype(BF) for b in below], axis=0)
    weight = jnp.transpose(weight_ref[...])

    for copy in fetches:
        copy.wait_recv()
    fetched = from_blocks(f_in)
    against = jnp.concatenate([fetched] + [doc] * (slots // ql), axis=0)
    rhs_t = (((1,), (1,)), ((), ()))
    top = lax.dot_general(query, against, rhs_t, preferred_element_type=F32)
    pos_row = jnp.sum(jnp.where(eye, top[:, slots:], 0.0), axis=0, keepdims=True)
    ex_out[0:ql, :] = top[:, :slots]
    ex_out[ql:, :] = jnp.broadcast_to(pos_row, (8, slots))
    s1 = alloc("s", n_mp - 1)
    t1 = alloc("r", n_mp - 1)
    shares = []
    for j in range(1, n_mp):
        copy = remote(ex_out, ex_in.at[m], s1 + j - 1, t1 + j - 1, mp=flip_bits(m, j))
        copy.start()
        shares.append(copy)
        sent.append(copy)
    spread(True, lambda copy: copy.start())

    def diagonal(level):
        return jnp.sum(jnp.where(eye, level, 0.0), axis=1, keepdims=True)

    def softmax(w, neg_score, pos_score):
        scale = scale_ref[w] * (1.0 / math.sqrt(bounds[w + 1]))
        neg_logit = jnp.where(named > 0.0, neg_score * scale, -1e30)
        pos_logit = pos_score * scale
        highest = jnp.maximum(jnp.max(neg_logit, axis=1, keepdims=True), pos_logit)
        neg_exp = named * jnp.exp(neg_logit - highest)
        pos_exp = jnp.exp(pos_logit - highest)
        denominator = jnp.sum(neg_exp, axis=1, keepdims=True) + pos_exp
        row_weight = weight[:, w : w + 1] * scale
        return (
            neg_exp * (row_weight / denominator),
            row_weight * (pos_exp / denominator - 1.0),
        )

    scores = lax.dot_general(q_prefix, against, rhs_t, preferred_element_type=F32)
    seg_neg = [None] * NW
    seg_pos = [None] * NW
    top_pos = diagonal(top[:, slots:])
    neg_run, pos_run = softmax(n_loc - 1, top[:, :slots], top_pos)
    seg_neg[n_loc - 1], seg_pos[n_loc - 1] = neg_run, pos_run
    for w in reversed(range(n_loc - 1)):
        level = scores[w * ql : (w + 1) * ql]
        neg_term, pos_term = softmax(w, level[:, :slots], diagonal(level[:, slots:]))
        neg_run, pos_run = neg_run + neg_term, pos_run + pos_term
        seg_neg[w], seg_pos[w] = neg_run, pos_run

    far = range(n_loc, NW)

    def inside_of(w, k):
        return jnp.where((k + 1) * cols <= bounds[w + 1], 1.0, 0.0)

    neg = {w: inside_of(w, m) * top[:, :slots] for w in far}
    pos = {w: inside_of(w, m) * top_pos for w in far}
    for j in range(1, n_mp):
        k = flip_bits(m, j)
        shares[j - 1].wait_recv()
        share = ex_in[k]
        other_neg = share[0:ql]
        other_pos = diagonal(jnp.broadcast_to(share[ql : ql + 1], (ql, slots)))
        for w in far:
            neg[w] = neg[w] + inside_of(w, k) * other_neg
            pos[w] = pos[w] + inside_of(w, k) * other_pos

    neg_run = jnp.zeros((ql, slots), F32)
    pos_run = jnp.zeros((ql, 1), F32)
    for w in reversed(far):
        neg_term, pos_term = softmax(w, neg[w], pos[w])
        neg_run, pos_run = neg_run + neg_term, pos_run + pos_term
        seg_neg[w], seg_pos[w] = neg_run, pos_run

    def local(values):
        low = [value + values[n_loc] for value in values[:n_loc]]
        mine = values[NW - 1]
        for s in reversed(range(n_loc, NW - 1)):
            mine = jnp.where((m + 1) * cols <= bounds[s + 1], values[s], mine)
        return [jnp.where(m == 0, low[0], mine)] + low[1:]

    columns = local(seg_pos)
    pos_cols = jnp.broadcast_to(columns[0], (ql, cols))
    for s in range(1, n_loc):
        here = jnp.logical_and(col_ids >= bounds[s], m == 0)
        pos_cols = jnp.where(here, columns[s], pos_cols)
    coef[...] = jnp.concatenate(local(seg_neg), axis=0).astype(BF)

    def part(s, n):
        return coef[s * ql : (s + n) * ql, :]

    @pl.when(m != 0)
    def _():
        term = lax.dot_general(part(0, 1), query, from_rows, preferred_element_type=F32)
        to_blocks(term, r_out)

    @pl.when(m == 0)
    def _():
        pieces = []
        for lo, hi, segs in groups:
            masked = [query[:, lo:hi] * seg[s][:, lo:hi].astype(BF) for s in segs]
            pieces.append(
                lax.dot_general(
                    part(segs[0], len(segs)),
                    jnp.concatenate(masked, axis=0),
                    from_rows,
                    preferred_element_type=F32,
                )
            )
        to_blocks(jnp.concatenate(pieces, axis=1), r_out)

    returns = exchange(lambda peer: r_out.at[peer], lambda peer: r_in.at[r])
    r_in[r] = r_out[r]

    @pl.when(m != 0)
    def _():
        term = jnp.dot(part(0, 1), fetched, preferred_element_type=F32)
        grads[r, 1] = (term + pos_cols * doc.astype(F32)).astype(BF)

    @pl.when(m == 0)
    def _():
        pieces = []
        for lo, hi, segs in groups:
            levels = jnp.dot(
                part(segs[0], len(segs)), fetched[:, lo:hi], preferred_element_type=F32
            )
            piece = levels[0:ql] * seg[segs[0]][:, lo:hi]
            for i in range(1, len(segs)):
                piece = piece + levels[i * ql : (i + 1) * ql] * seg[segs[i]][:, lo:hi]
            pieces.append(piece)
        term = jnp.concatenate(pieces, axis=1)
        grads[r, 1] = (term + pos_cols * doc.astype(F32)).astype(BF)

    rows = ql // parts

    def gather(h):
        return Gather(lambda o, c: grads.at[o, h, pl.ds(c * rows, rows)], parts)

    gather_q = gather(1)
    gather_q.start()

    def partial_start(h, between):
        s = alloc("s", n_mp - 1)
        t = alloc("r", n_mp - 1)
        copies = []
        value = grads[r, h]
        for j in [*range(2, n_mp), 1]:
            k = flip_bits(m, j)
            term = lax.dot_general(value, head_rows(k), rhs_t, preferred_element_type=F32)
            part_out[h, j - 1] = term.astype(BF)
            copy = remote(
                part_out.at[h, j - 1], part_in.at[h, j - 1], s + j - 1, t + j - 1, mp=k
            )
            copy.start()
            copies.append(copy)
            sent.append(copy)
            between(len(copies))
        mine = lax.dot_general(value, head_rows(m), rhs_t, preferred_element_type=F32)
        return copies, mine

    def partial_end(h, copies, mine):
        for j, copy in zip([*range(2, n_mp), 1], copies):
            copy.wait_recv()
            mine = mine + part_in[h, j - 1].astype(F32)
        return mine.astype(BF)

    part_q = partial_start(1, lambda n: None)
    hand_pass(0)
    hand_start(1)
    gather_q.forward(1)
    for copy in returns:
        copy.wait_recv()
    doc_back = jnp.dot(sel_t, from_blocks(r_in), preferred_element_type=F32)
    grads[r, 0] = (doc_back + pos_cols * query.astype(F32)).astype(BF)
    gather_d = gather(0)
    gather_d.start()
    gather_q.forward(*range(2, half - 1))
    part_d = partial_start(0, lambda n: None)
    gather_d.forward(1)
    gather_q.forward(*range(max(half - 1, 2), half))
    gather_d.forward(*range(2, half - 1))
    hand_pass(1)
    qg_ref[...] = partial_end(1, *part_q)
    hand_end(0)
    hand_end(1)
    gather_q.drain()
    gather_d.forward(*range(max(half - 1, 2), half))
    dg_ref[...] = partial_end(0, *part_d)
    for k in range(half):
        line = lax.rem(place + k, half)
        gather_q.finish(line)
        gather_d.finish(line)
        both = jnp.concatenate([rows_t[0, line], rows_t[1, line]], axis=1)
        term = jnp.dot(
            both,
            grads[pl.ds(line * 2, 2)].reshape(4 * ql, cols),
            preferred_element_type=F32,
        )
        if k == 0:
            hg_ref[...] = term
        else:
            hg_ref[...] += term

    for copy in sent:
        copy.wait_send()
    gather_d.drain()
    spread(False, lambda copy: copy.wait_send())
    spread(True, lambda copy: copy.wait_send())

    @pl.when(m == keeper)
    def _():
        for copy in halves[0] + halves[1]:
            copy.wait_send()

    @pl.when(passes)
    def _():
        halves[0][-1].wait_send()
        halves[1][-1].wait_send()


def hand_on(*refs):
    for src, dst in zip(refs[: len(refs) // 2], refs[len(refs) // 2 :]):
        dst[...] = src[...]


def solution(mesh):
    n_dp = mesh.shape["dp"]
    n_mp = mesh.shape["mp"]

    def on_device(query_rows, doc_rows, head, logit_scale, loss_grad, shortlist, send_rows):
        ql, cols = query_rows.shape
        total = n_mp * cols
        slots = send_rows.shape[1]
        blk = slots // n_dp
        chunk = total // n_dp
        n_loc = local_segments(width_bounds(total), cols)
        n_send = 7 * (n_mp - 1) + n_dp // n_mp + 2 * (n_dp - 1) + 2 * PARTS * (2 * n_dp - 1)
        n_recv = 5 * (n_mp - 1) + n_dp + 2 * (n_dp - 1) + 2 + 2 * PARTS * n_dp
        vmem = pl.BlockSpec(memory_space=pltpu.VMEM)
        shapes = (
            jax.ShapeDtypeStruct((ql, cols), BF),
            jax.ShapeDtypeStruct((ql, cols), BF),
            jax.ShapeDtypeStruct((chunk, cols), F32),
        )
        found = pl.pallas_call(
            functools.partial(kernel, n_dp, n_mp),
            out_shape=shapes,
            in_specs=[pl.BlockSpec(memory_space=pltpu.HBM)] * 7,
            out_specs=(vmem, vmem, vmem),
            scratch_shapes=[
                pltpu.VMEM((ql, cols), BF),
                pltpu.VMEM((ql, cols), BF),
                pltpu.SMEM(logit_scale.shape, F32),
                pltpu.VMEM(loss_grad.shape[::-1], F32),
                pltpu.VMEM(shortlist.shape, jnp.int32),
                pltpu.VMEM(send_rows.shape, jnp.int32),
                pltpu.VMEM((total, cols), BF),
                pltpu.VMEM((n_mp, 2, ql, cols), BF),
                pltpu.VMEM((cols, 2 * ql), BF),
                pltpu.VMEM((2, n_dp // 2, chunk, 2 * ql), BF),
                pltpu.VMEM((n_dp, blk, cols), BF),
                pltpu.VMEM((n_dp, blk, cols), BF),
                pltpu.VMEM((ql + 8, slots), F32),
                pltpu.VMEM((n_mp, ql + 8, slots), F32),
                pltpu.VMEM((n_loc * ql, slots), BF),
                pltpu.VMEM((n_dp, blk, cols), BF),
                pltpu.VMEM((n_dp, blk, cols), BF),
                pltpu.VMEM((n_dp, 2, ql, cols), BF),
                pltpu.VMEM((2, n_mp - 1, ql, cols), BF),
                pltpu.VMEM((2, n_mp - 1, ql, cols), BF),
                pltpu.VMEM((slots, cols), F32),
                pltpu.SemaphoreType.DMA((n_send,)),
                pltpu.SemaphoreType.DMA((n_recv,)),
                pltpu.SemaphoreType.DMA((8,)),
            ],
            compiler_params=pltpu.CompilerParams(
                collective_id=0, has_side_effects=True, vmem_limit_bytes=48 << 20
            ),
        )(
            *[
                pltpu.with_memory_space_constraint(x, pltpu.HBM)
                for x in (
                    query_rows,
                    doc_rows,
                    head,
                    logit_scale,
                    loss_grad.T,
                    shortlist,
                    send_rows,
                )
            ]
        )
        return pl.pallas_call(
            hand_on,
            out_shape=shapes,
            in_specs=[vmem] * 3,
            out_specs=(vmem,) * 3,
            compiler_params=pltpu.CompilerParams(vmem_limit_bytes=8 << 20),
        )(*found)

    return jax.shard_map(
        on_device,
        mesh=mesh,
        in_specs=(
            P("dp", "mp"),
            P("dp", "mp"),
            P(None, "mp"),
            P(),
            P("dp", None),
            P("dp", None),
            P("dp", None),
        ),
        out_specs=(P("dp", "mp"), P("dp", "mp"), P("dp", "mp")),
        check_vma=False,
    )
```

```python
import functools
import math

import jax
import jax.numpy as jnp
from jax import lax
from jax.experimental import pallas as pl
from jax.experimental.pallas import tpu as pltpu
from jax.sharding import PartitionSpec as P

NW = 7
PARTS = 2
MESH = pl.DeviceIdType.MESH
BF = jnp.bfloat16
F32 = jnp.float32


def width_bounds(feature_total):
    return [0] + [feature_total // 2 ** (NW - 1 - level) for level in range(NW)]


def local_segments(bounds, cols):
    return sum(bound <= cols for bound in bounds[1:])


def flip_bits(value, mask):
    bit = 1
    while bit <= mask:
        if mask & bit:
            value = value + bit - 2 * bit * lax.rem(lax.div(value, bit), 2)
        bit *= 2
    return value


def kernel(
    n_dp,
    n_mp,
    q_hbm,
    d_hbm,
    head_hbm,
    scale_hbm,
    weight_hbm,
    short_hbm,
    rows_hbm,
    qg_ref,
    dg_ref,
    hg_ref,
    q_ref,
    d_ref,
    scale_ref,
    weight_ref,
    short_ref,
    rows_ref,
    head,
    whole,
    own_t,
    rows_t,
    f_out,
    f_in,
    ex_out,
    ex_in,
    coef,
    r_out,
    r_in,
    grads,
    part_out,
    part_in,
    flat,
    ssem,
    rsem,
    lsem,
):
    ql, cols = q_ref.shape
    total = n_mp * cols
    slots = rows_ref.shape[1]
    blk = slots // n_dp
    chunk = total // n_dp
    per_mp = n_dp // n_mp
    half = n_dp // 2
    bounds = width_bounds(total)
    n_loc = local_segments(bounds, cols)
    r = lax.axis_index("dp")
    m = lax.axis_index("mp")
    partner = flip_bits(r, 1)

    counts = {}

    def alloc(kind, n):
        start = counts.get(kind, 0)
        counts[kind] = start + n
        return start

    def remote(src, dst, s, t, **where):
        return pltpu.make_async_remote_copy(
            src_ref=src,
            dst_ref=dst,
            send_sem=ssem.at[s],
            recv_sem=rsem.at[t],
            device_id=where,
            device_id_type=MESH,
        )

    loads = [
        pltpu.make_async_copy(src, dst, lsem.at[2 + i])
        for i, (src, dst) in enumerate(
            [
                (d_hbm, d_ref),
                (q_hbm, q_ref),
                (rows_hbm, rows_ref),
                (short_hbm, short_ref),
                (weight_hbm, weight_ref),
                (scale_hbm, scale_ref),
            ]
        )
    ]
    for copy in loads:
        copy.start()
    head_copy = pltpu.make_async_copy(head_hbm, head, lsem.at[0])
    head_copy.start()
    barrier = pltpu.get_barrier_semaphore()
    for j in range(1, n_mp):
        pl.semaphore_signal(
            barrier, inc=1, device_id={"mp": flip_bits(m, j)}, device_id_type=MESH
        )
    for k in range(1, n_dp):
        pl.semaphore_signal(
            barrier, inc=1, device_id={"dp": lax.rem(r + k, n_dp)}, device_id_type=MESH
        )
    for copy in loads:
        copy.wait()
    pl.semaphore_wait(barrier, n_mp - 1 + n_dp - 1)

    parts = PARTS

    def sent_rows(s, n):
        ref = head.at[pl.ds(0, n)]
        remote(ref, ref, s, 0, dp=partner).wait_send()

    def came_rows(t, n):
        ref = head.at[pl.ds(0, n)]
        remote(ref, ref, 0, t, dp=partner).wait_recv()

    def sent_blocks(pair):
        ref = f_in.at[pl.ds(0, n_dp - 1)]
        remote(ref, ref, *pair, dp=partner).wait_send()

    def came_blocks(pair):
        ref = f_in.at[pl.ds(0, n_dp - 1)]
        remote(ref, ref, *pair, dp=partner).wait_recv()

    s0 = alloc("s", 1)
    t0 = alloc("r", 2 * (n_mp - 1))
    row_copies = []
    for h, ref in enumerate((d_ref, q_ref)):
        base = h * (n_mp - 1) - 1
        copies = {}
        for j in [*range(2, n_mp, 2), 1]:
            copies[j] = remote(
                ref, whole.at[m, h], s0, t0 + base + j, mp=flip_bits(m, j)
            )
            copies[j].start()
        for j in range(2, n_mp, 2):
            k = flip_bits(m, j)
            copies[j + 1] = remote(
                whole.at[k, h],
                whole.at[k, h],
                s0,
                t0 + base + j + 1,
                mp=flip_bits(m, 1),
            )
        row_copies.append(copies)

    def exchange(out, into):
        s = alloc("s", 1)
        t = alloc("r", 1)
        for k in range(1, n_dp):
            peer = lax.rem(r + k, n_dp)
            remote(out(peer), into(peer), s, t, dp=peer).start()
        return s, t

    own = jnp.concatenate([d_ref[...], q_ref[...]], axis=0)
    own_t[...] = jnp.transpose(own)
    s_t = alloc("s", per_mp)
    t_t = alloc("r", 2)
    place = lax.div(r, 2)
    side = lax.rem(r, 2)
    keeper = lax.div(r, per_mp)

    def spread(late, step):
        for i in range(per_mp // 2):
            c = 2 * i + (1 - side if late else side)
            target = m * per_mp + c
            copy = remote(
                own_t.at[pl.ds(pl.multiple_of(c * chunk, 16), chunk)],
                rows_t.at[side, place],
                s_t + 2 * i + int(late),
                t_t + int(late),
                dp=target,
            )
            if late:
                step(copy)
            else:
                pl.when(target != r)(functools.partial(step, copy))

    spread(False, lambda copy: copy.start())

    @pl.when(m == keeper)
    def _():
        c = lax.rem(r, per_mp)
        rows_t[side, place] = own_t[pl.ds(pl.multiple_of(c * chunk, 16), chunk), :]

    s_f = alloc("s", 2)
    t_f = alloc("r", 2)
    same = lax.rem(m, 2) == lax.rem(keeper, 2)
    passes = jnp.logical_and(same, m != keeper)

    def hand_over(late):
        ref = rows_t.at[1 - side if late else side]
        return [
            remote(ref, ref, s_f + int(late), t_f + int(late), mp=flip_bits(m, j))
            for j in [*range(2, n_mp, 2), 1]
        ]

    halves = [hand_over(False), hand_over(True)]

    def hand_start(late):
        @pl.when(m == keeper)
        def _():
            n = half if late else half - 1
            came_rows(t_t + int(late), n * chunk * 2 * ql // cols)
            for copy in halves[late]:
                copy.start()

    def hand_pass(late):
        @pl.when(passes)
        def _():
            halves[late][-1].wait_recv()
            halves[late][-1].start()

    def hand_end(late):
        @pl.when(jnp.logical_not(same))
        def _():
            halves[late][-1].wait_recv()

    head_copy.wait()

    def head_rows(k):
        return head[pl.ds(pl.multiple_of(k * cols, cols), cols), :]

    def project(h, ref):
        copies = row_copies[h]
        acc = jnp.dot(ref[...], head_rows(m), preferred_element_type=F32)
        for j in range(1, n_mp, 2):
            for i in [j] if j == 1 else [j - 1, j]:
                k = flip_bits(m, i)
                copies[i].wait_recv()
                if i % 2 == 0:
                    copies[i + 1].start()
                acc = acc + jnp.dot(whole[k, h], head_rows(k), preferred_element_type=F32)
        return acc.astype(BF)

    s_g = alloc("s", 2)
    t_g = alloc("r", half)

    class Gather:
        def __init__(self, h):
            self.h = h
            self.t = alloc("r", parts * half)
            self.own = [
                ([self.copy(r, c, dz) for c in range(parts)], self.within(dz))
                for dz in (-1, 1)
            ]
            self.across = [self.copy(r, c, 0) for c in range(parts)]
            self.hops = {}
            for d in range(1, half):
                self.hops[d] = []
                for dz in (-1, 1):
                    origin = lax.rem(r - 2 * dz * d + 2 * n_dp, n_dp)
                    steps = [
                        (self.copy(origin, c, dz), self.copy(origin, c, 0))
                        for c in range(parts)
                    ]
                    self.hops[d].append((self.within(-dz * d), self.within(dz), steps))

        def within(self, step):
            return place + step >= 0 if step < 0 else place + step < half

        def copy(self, origin, c, dz):
            rows = ql // parts
            ref = grads.at[origin, self.h, pl.ds(c * rows, rows)]
            line = lax.div(origin, 2)
            target = lax.rem(r + 2 * dz + n_dp, n_dp) if dz else partner
            t = self.t + line * parts + c if dz else t_g + line
            return remote(ref, ref, s_g + self.h, t, dp=target)

        def start(self):
            for copies, inside in self.own:

                @pl.when(inside)
                def _(copies=copies):
                    for copy in copies:
                        copy.start()

            for copy in self.across:
                copy.start()

        def forward(self, *hops):
            for d in hops:
                for there, further, steps in self.hops[d]:

                    @pl.when(there)
                    def _(further=further, steps=steps):
                        for relay, over in steps:
                            relay.wait_recv()
                            pl.when(further)(relay.start)
                            over.start()

    slot_ids = lax.broadcasted_iota(jnp.int32, (ql, slots), 1)
    row_ids = lax.broadcasted_iota(jnp.int32, (ql, slots), 0)
    eye = slot_ids == row_ids
    from_rows = (((0,), (0,)), ((), ()))

    sel_t32 = jnp.where(rows_ref[...] == row_ids, 1.0, 0.0)
    sel_t = sel_t32.astype(BF)
    sel = jnp.transpose(sel_t32).astype(BF)
    doc = project(0, d_ref)

    def to_blocks(values, out):
        if blk % 16 == 0:
            out[...] = values.astype(BF).reshape(n_dp, blk, cols)
        else:
            flat[...] = values
            for p in range(n_dp):
                out[p] = flat[p * blk : (p + 1) * blk, :].astype(BF)

    def from_blocks(buf):
        if blk % 16 == 0:
            return buf[...].reshape(slots, cols)
        for p in range(n_dp):
            flat[p * blk : (p + 1) * blk, :] = buf[p].astype(F32)
        return flat[...].astype(BF)

    to_blocks(jnp.dot(sel, doc, preferred_element_type=F32), f_out)
    fetches = exchange(lambda peer: f_out.at[peer], lambda peer: f_in.at[r])
    f_in[r] = f_out[r]
    query = project(1, q_ref)
    hand_start(0)

    short = short_ref[...]
    named = jnp.zeros((ql, slots), F32)
    for n in range(short.shape[1]):
        named = named + jnp.where(short[:, n : n + 1] == slot_ids, 1.0, 0.0)

    col_ids = lax.broadcasted_iota(jnp.int32, (1, cols), 1)
    seg = [
        jnp.where(jnp.logical_and(col_ids >= bounds[s], col_ids < bounds[s + 1]), 1.0, 0.0)
        for s in range(n_loc)
    ]
    cut = min(256, cols)
    groups = [
        (lo, hi, [s for s in range(n_loc) if bounds[s] < hi and bounds[s + 1] > lo])
        for lo, hi in ((0, cut), (cut, cols))
        if lo < hi
    ]
    below = [jnp.where(col_ids < bounds[w + 1], 1.0, 0.0) for w in range(n_loc - 1)]
    q_prefix = jnp.concatenate([query * b.astype(BF) for b in below], axis=0)
    weight = jnp.transpose(weight_ref[...])

    came_blocks(fetches)
    fetched = from_blocks(f_in)
    against = jnp.concatenate([fetched] + [doc] * (slots // ql), axis=0)
    rhs_t = (((1,), (1,)), ((), ()))
    top = lax.dot_general(query, against, rhs_t, preferred_element_type=F32)
    pos_row = jnp.sum(jnp.where(eye, top[:, slots:], 0.0), axis=0, keepdims=True)
    ex_out[0:ql, :] = top[:, :slots]
    ex_out[ql:, :] = jnp.broadcast_to(pos_row, (8, slots))
    s1 = alloc("s", 1)
    t1 = alloc("r", n_mp - 1)
    shares = []
    for j in range(1, n_mp):
        copy = remote(ex_out, ex_in.at[m], s1, t1 + j - 1, mp=flip_bits(m, j))
        copy.start()
        shares.append(copy)
    spread(True, lambda copy: copy.start())

    def diagonal(level):
        return jnp.sum(jnp.where(eye, level, 0.0), axis=1, keepdims=True)

    def softmax(w, neg_score, pos_score):
        scale = scale_ref[w] * (1.0 / math.sqrt(bounds[w + 1]))
        neg_logit = jnp.where(named > 0.0, neg_score * scale, -1e30)
        pos_logit = pos_score * scale
        highest = jnp.maximum(jnp.max(neg_logit, axis=1, keepdims=True), pos_logit)
        neg_exp = named * jnp.exp(neg_logit - highest)
        pos_exp = jnp.exp(pos_logit - highest)
        denominator = jnp.sum(neg_exp, axis=1, keepdims=True) + pos_exp
        row_weight = weight[:, w : w + 1] * scale
        return (
            neg_exp * (row_weight / denominator),
            row_weight * (pos_exp / denominator - 1.0),
        )

    scores = lax.dot_general(q_prefix, against, rhs_t, preferred_element_type=F32)
    seg_neg = [None] * NW
    seg_pos = [None] * NW
    top_pos = diagonal(top[:, slots:])
    neg_run, pos_run = softmax(n_loc - 1, top[:, :slots], top_pos)
    seg_neg[n_loc - 1], seg_pos[n_loc - 1] = neg_run, pos_run
    for w in reversed(range(n_loc - 1)):
        level = scores[w * ql : (w + 1) * ql]
        neg_term, pos_term = softmax(w, level[:, :slots], diagonal(level[:, slots:]))
        neg_run, pos_run = neg_run + neg_term, pos_run + pos_term
        seg_neg[w], seg_pos[w] = neg_run, pos_run

    far = range(n_loc, NW)

    def inside_of(w, k):
        return jnp.where((k + 1) * cols <= bounds[w + 1], 1.0, 0.0)

    neg = {w: inside_of(w, m) * top[:, :slots] for w in far}
    pos = {w: inside_of(w, m) * top_pos for w in far}
    for j in range(1, n_mp):
        k = flip_bits(m, j)
        shares[j - 1].wait_recv()
        share = ex_in[k]
        other_neg = share[0:ql]
        other_pos = diagonal(jnp.broadcast_to(share[ql : ql + 1], (ql, slots)))
        for w in far:
            neg[w] = neg[w] + inside_of(w, k) * other_neg
            pos[w] = pos[w] + inside_of(w, k) * other_pos

    neg_run = jnp.zeros((ql, slots), F32)
    pos_run = jnp.zeros((ql, 1), F32)
    for w in reversed(far):
        neg_term, pos_term = softmax(w, neg[w], pos[w])
        neg_run, pos_run = neg_run + neg_term, pos_run + pos_term
        seg_neg[w], seg_pos[w] = neg_run, pos_run

    def local(values):
        low = [value + values[n_loc] for value in values[:n_loc]]
        mine = values[NW - 1]
        for s in reversed(range(n_loc, NW - 1)):
            mine = jnp.where((m + 1) * cols <= bounds[s + 1], values[s], mine)
        return [jnp.where(m == 0, low[0], mine)] + low[1:]

    columns = local(seg_pos)
    pos_cols = jnp.broadcast_to(columns[0], (ql, cols))
    for s in range(1, n_loc):
        here = jnp.logical_and(col_ids >= bounds[s], m == 0)
        pos_cols = jnp.where(here, columns[s], pos_cols)
    coef[...] = jnp.concatenate(local(seg_neg), axis=0).astype(BF)

    def part(s, n):
        return coef[s * ql : (s + n) * ql, :]

    @pl.when(m != 0)
    def _():
        term = lax.dot_general(part(0, 1), query, from_rows, preferred_element_type=F32)
        to_blocks(term, r_out)

    @pl.when(m == 0)
    def _():
        pieces = []
        for lo, hi, segs in groups:
            masked = [query[:, lo:hi] * seg[s][:, lo:hi].astype(BF) for s in segs]
            pieces.append(
                lax.dot_general(
                    part(segs[0], len(segs)),
                    jnp.concatenate(masked, axis=0),
                    from_rows,
                    preferred_element_type=F32,
                )
            )
        to_blocks(jnp.concatenate(pieces, axis=1), r_out)

    returns = exchange(lambda peer: r_out.at[peer], lambda peer: r_in.at[r])
    r_in[r] = r_out[r]

    @pl.when(m != 0)
    def _():
        term = jnp.dot(part(0, 1), fetched, preferred_element_type=F32)
        grads[r, 1] = (term + pos_cols * doc.astype(F32)).astype(BF)

    @pl.when(m == 0)
    def _():
        pieces = []
        for lo, hi, segs in groups:
            levels = jnp.dot(
                part(segs[0], len(segs)), fetched[:, lo:hi], preferred_element_type=F32
            )
            piece = levels[0:ql] * seg[segs[0]][:, lo:hi]
            for i in range(1, len(segs)):
                piece = piece + levels[i * ql : (i + 1) * ql] * seg[segs[i]][:, lo:hi]
            pieces.append(piece)
        term = jnp.concatenate(pieces, axis=1)
        grads[r, 1] = (term + pos_cols * doc.astype(F32)).astype(BF)

    gather_q = Gather(1)
    gather_q.start()

    s_p = alloc("s", 1)
    t_p = alloc("r", 2)

    def partial_start(h):
        value = grads[r, h]
        for j in [*range(2, n_mp), 1]:
            k = flip_bits(m, j)
            term = lax.dot_general(value, head_rows(k), rhs_t, preferred_element_type=F32)
            part_out[h, j - 1] = term.astype(BF)
            remote(part_out.at[h, j - 1], part_in.at[h, j - 1], s_p, t_p + h, mp=k).start()
        return lax.dot_general(value, head_rows(m), rhs_t, preferred_element_type=F32)

    def partial_end(h, mine):
        came_rows(t_p + h, (n_mp - 1) * ql)
        for j in range(1, n_mp):
            mine = mine + part_in[h, j - 1].astype(F32)
        return mine.astype(BF)

    part_q = partial_start(1)
    hand_pass(0)
    hand_start(1)
    came_blocks(returns)
    doc_back = jnp.dot(sel_t, from_blocks(r_in), preferred_element_type=F32)
    grads[r, 0] = (doc_back + pos_cols * query.astype(F32)).astype(BF)
    gather_d = Gather(0)
    gather_d.start()
    gather_q.forward(1)
    part_d = partial_start(0)
    gather_q.forward(*range(2, half - 1))
    gather_d.forward(1)
    gather_q.forward(*range(max(half - 1, 2), half))
    gather_d.forward(*range(2, half - 1))
    hand_pass(1)
    qg_ref[...] = partial_end(1, part_q)
    hand_end(0)
    hand_end(1)
    gather_d.forward(*range(max(half - 1, 2), half))
    dg_ref[...] = partial_end(0, part_d)
    for k in range(half):
        line = lax.rem(place + k, half)
        came_rows(t_g + line, 2 * ql)
        both = jnp.concatenate([rows_t[0, line], rows_t[1, line]], axis=1)
        term = jnp.dot(
            both,
            grads[pl.ds(line * 2, 2)].reshape(4 * ql, cols),
            preferred_element_type=F32,
        )
        if k == 0:
            hg_ref[...] = term
        else:
            hg_ref[...] += term

    inner = jnp.logical_and(place > 0, place < half - 1)

    @pl.when(inner)
    def _():
        for h in (0, 1):
            sent_rows(s_g + h, ql * (2 * half + 1))

    @pl.when(jnp.logical_not(inner))
    def _():
        for h in (0, 1):
            sent_rows(s_g + h, ql * (half + 1))

    sent_rows(s0, 2 * (n_mp - 1) * ql)
    sent_blocks(fetches)
    sent_blocks(returns)
    sent_rows(s_p, 2 * (n_mp - 1) * ql)
    others = ex_in.at[pl.ds(0, n_mp - 1)]
    remote(others, others, s1, 0, dp=partner).wait_send()
    spread(False, lambda copy: copy.wait_send())
    spread(True, lambda copy: copy.wait_send())
    half_rows = half * chunk * 2 * ql // cols

    @pl.when(m == keeper)
    def _():
        for late in (0, 1):
            sent_rows(s_f + late, n_mp // 2 * half_rows)

    @pl.when(passes)
    def _():
        for late in (0, 1):
            sent_rows(s_f + late, half_rows)


def hand_on(*refs):
    for src, dst in zip(refs[: len(refs) // 2], refs[len(refs) // 2 :]):
        dst[...] = src[...]


def solution(mesh):
    n_dp = mesh.shape["dp"]
    n_mp = mesh.shape["mp"]

    def on_device(query_rows, doc_rows, head, logit_scale, loss_grad, shortlist, send_rows):
        ql, cols = query_rows.shape
        total = n_mp * cols
        slots = send_rows.shape[1]
        blk = slots // n_dp
        chunk = total // n_dp
        n_loc = local_segments(width_bounds(total), cols)
        n_send = 9 + n_dp // n_mp
        n_recv = 3 * (n_mp - 1) + 8 + n_dp // 2 + PARTS * n_dp
        vmem = pl.BlockSpec(memory_space=pltpu.VMEM)
        shapes = (
            jax.ShapeDtypeStruct((ql, cols), BF),
            jax.ShapeDtypeStruct((ql, cols), BF),
            jax.ShapeDtypeStruct((chunk, cols), F32),
        )
        found = pl.pallas_call(
            functools.partial(kernel, n_dp, n_mp),
            out_shape=shapes,
            in_specs=[pl.BlockSpec(memory_space=pltpu.HBM)] * 7,
            out_specs=(vmem, vmem, vmem),
            scratch_shapes=[
                pltpu.VMEM((ql, cols), BF),
                pltpu.VMEM((ql, cols), BF),
                pltpu.SMEM(logit_scale.shape, F32),
                pltpu.VMEM(loss_grad.shape[::-1], F32),
                pltpu.VMEM(shortlist.shape, jnp.int32),
                pltpu.VMEM(send_rows.shape, jnp.int32),
                pltpu.VMEM((total, cols), BF),
                pltpu.VMEM((n_mp, 2, ql, cols), BF),
                pltpu.VMEM((cols, 2 * ql), BF),
                pltpu.VMEM((2, n_dp // 2, chunk, 2 * ql), BF),
                pltpu.VMEM((n_dp, blk, cols), BF),
                pltpu.VMEM((n_dp, blk, cols), BF),
                pltpu.VMEM((ql + 8, slots), F32),
                pltpu.VMEM((n_mp, ql + 8, slots), F32),
                pltpu.VMEM((n_loc * ql, slots), BF),
                pltpu.VMEM((n_dp, blk, cols), BF),
                pltpu.VMEM((n_dp, blk, cols), BF),
                pltpu.VMEM((n_dp, 2, ql, cols), BF),
                pltpu.VMEM((2, n_mp - 1, ql, cols), BF),
                pltpu.VMEM((2, n_mp - 1, ql, cols), BF),
                pltpu.VMEM((slots, cols), F32),
                pltpu.SemaphoreType.DMA((n_send,)),
                pltpu.SemaphoreType.DMA((n_recv,)),
                pltpu.SemaphoreType.DMA((8,)),
            ],
            compiler_params=pltpu.CompilerParams(
                collective_id=0, has_side_effects=True, vmem_limit_bytes=48 << 20
            ),
        )(
            *[
                pltpu.with_memory_space_constraint(x, pltpu.HBM)
                for x in (
                    query_rows,
                    doc_rows,
                    head,
                    logit_scale,
                    loss_grad.T,
                    shortlist,
                    send_rows,
                )
            ]
        )
        return pl.pallas_call(
            hand_on,
            out_shape=shapes,
            in_specs=[vmem] * 3,
            out_specs=(vmem,) * 3,
            compiler_params=pltpu.CompilerParams(vmem_limit_bytes=8 << 20),
        )(*found)

    return jax.shard_map(
        on_device,
        mesh=mesh,
        in_specs=(
            P("dp", "mp"),
            P("dp", "mp"),
            P(None, "mp"),
            P(),
            P("dp", None),
            P("dp", None),
            P("dp", None),
        ),
        out_specs=(P("dp", "mp"), P("dp", "mp"), P("dp", "mp")),
        check_vma=False,
    )
```

```python
import functools
import math

import jax
import jax.numpy as jnp
from jax import lax
from jax.experimental import pallas as pl
from jax.experimental.pallas import tpu as pltpu
from jax.sharding import PartitionSpec as P

NW = 7
PARTS = 2
MESH = pl.DeviceIdType.MESH
BF = jnp.bfloat16
F32 = jnp.float32


def width_bounds(feature_total):
    return [0] + [feature_total // 2 ** (NW - 1 - level) for level in range(NW)]


def local_segments(bounds, cols):
    return sum(bound <= cols for bound in bounds[1:])


def flip_bits(value, mask):
    bit = 1
    while bit <= mask:
        if mask & bit:
            value = value + bit - 2 * bit * lax.rem(lax.div(value, bit), 2)
        bit *= 2
    return value


def kernel(
    n_dp,
    n_mp,
    q_hbm,
    d_hbm,
    head_hbm,
    scale_hbm,
    weight_hbm,
    short_hbm,
    rows_hbm,
    qg_ref,
    dg_ref,
    hg_ref,
    q_ref,
    d_ref,
    scale_ref,
    weight_ref,
    short_ref,
    rows_ref,
    head,
    whole,
    own_t,
    rows_t,
    f_out,
    f_in,
    ex_out,
    ex_in,
    coef,
    r_out,
    r_in,
    grads,
    part_out,
    part_in,
    flat,
    ssem,
    rsem,
    lsem,
):
    ql, cols = q_ref.shape
    total = n_mp * cols
    slots = rows_ref.shape[1]
    blk = slots // n_dp
    chunk = total // n_dp
    per_mp = n_dp // n_mp
    half = n_dp // 2
    bounds = width_bounds(total)
    n_loc = local_segments(bounds, cols)
    r = lax.axis_index("dp")
    m = lax.axis_index("mp")
    partner = flip_bits(r, 1)

    counts = {}

    def alloc(kind, n):
        start = counts.get(kind, 0)
        counts[kind] = start + n
        return start

    def remote(src, dst, s, t, **where):
        return pltpu.make_async_remote_copy(
            src_ref=src,
            dst_ref=dst,
            send_sem=ssem.at[s],
            recv_sem=rsem.at[t],
            device_id=where,
            device_id_type=MESH,
        )

    loads = [
        pltpu.make_async_copy(src, dst, lsem.at[2 + i])
        for i, (src, dst) in enumerate(
            [
                (d_hbm, d_ref),
                (q_hbm, q_ref),
                (rows_hbm, rows_ref),
                (short_hbm, short_ref),
                (weight_hbm, weight_ref),
                (scale_hbm, scale_ref),
            ]
        )
    ]
    for copy in loads:
        copy.start()
    head_copy = pltpu.make_async_copy(head_hbm, head, lsem.at[0])
    head_copy.start()
    barrier = pltpu.get_barrier_semaphore()
    for j in range(1, n_mp):
        pl.semaphore_signal(
            barrier, inc=1, device_id={"mp": flip_bits(m, j)}, device_id_type=MESH
        )
    for k in range(1, n_dp):
        pl.semaphore_signal(
            barrier, inc=1, device_id={"dp": lax.rem(r + k, n_dp)}, device_id_type=MESH
        )
    for copy in loads:
        copy.wait()
    pl.semaphore_wait(barrier, n_mp - 1 + n_dp - 1)

    parts = PARTS

    def sent_rows(s, n):
        ref = head.at[pl.ds(0, n)]
        remote(ref, ref, s, 0, dp=partner).wait_send()

    def came_rows(t, n):
        ref = head.at[pl.ds(0, n)]
        remote(ref, ref, 0, t, dp=partner).wait_recv()

    def sent_blocks(pair):
        ref = f_in.at[pl.ds(0, n_dp - 1)]
        remote(ref, ref, *pair, dp=partner).wait_send()

    def came_blocks(pair):
        ref = f_in.at[pl.ds(0, n_dp - 1)]
        remote(ref, ref, *pair, dp=partner).wait_recv()

    s0 = alloc("s", 1)
    t0 = alloc("r", 2 * (n_mp - 1))
    row_copies = []
    for h, ref in enumerate((d_ref, q_ref)):
        base = h * (n_mp - 1) - 1
        copies = {}
        for j in [*range(3, n_mp, 2), 1]:
            copies[j] = remote(
                ref, whole.at[m, h], s0, t0 + base + j, mp=flip_bits(m, j)
            )
            copies[j].start()
        for j in range(3, n_mp, 2):
            k = flip_bits(m, j)
            copies[j - 1] = remote(
                whole.at[k, h],
                whole.at[k, h],
                s0,
                t0 + base + j - 1,
                mp=flip_bits(m, 1),
            )
        row_copies.append(copies)

    def exchange(out, into):
        s = alloc("s", 1)
        t = alloc("r", 1)
        for k in range(1, n_dp):
            peer = lax.rem(r + k, n_dp)
            remote(out(peer), into(peer), s, t, dp=peer).start()
        return s, t

    own = jnp.concatenate([d_ref[...], q_ref[...]], axis=0)
    own_t[...] = jnp.transpose(own)
    s_t = alloc("s", per_mp)
    t_t = alloc("r", 2)
    place = lax.div(r, 2)
    side = lax.rem(r, 2)
    keeper = lax.div(r, per_mp)

    def spread(late, step):
        for i in range(per_mp // 2):
            c = 2 * i + (1 - side if late else side)
            target = m * per_mp + c
            copy = remote(
                own_t.at[pl.ds(pl.multiple_of(c * chunk, 16), chunk)],
                rows_t.at[side, place],
                s_t + 2 * i + int(late),
                t_t + int(late),
                dp=target,
            )
            if late:
                step(copy)
            else:
                pl.when(target != r)(functools.partial(step, copy))

    spread(False, lambda copy: copy.start())

    @pl.when(m == keeper)
    def _():
        c = lax.rem(r, per_mp)
        rows_t[side, place] = own_t[pl.ds(pl.multiple_of(c * chunk, 16), chunk), :]

    s_f = alloc("s", 2)
    t_f = alloc("r", 2)
    same = lax.rem(m, 2) == lax.rem(keeper, 2)
    passes = jnp.logical_and(same, m != keeper)

    def hand_over(late):
        ref = rows_t.at[1 - side if late else side]
        return [
            remote(ref, ref, s_f + int(late), t_f + int(late), mp=flip_bits(m, j))
            for j in [*range(2, n_mp, 2), 1]
        ]

    halves = [hand_over(False), hand_over(True)]

    def hand_start(late):
        @pl.when(m == keeper)
        def _():
            n = half if late else half - 1
            came_rows(t_t + int(late), n * chunk * 2 * ql // cols)
            for copy in halves[late]:
                copy.start()

    def hand_pass(late):
        @pl.when(passes)
        def _():
            halves[late][-1].wait_recv()
            halves[late][-1].start()

    def hand_end(late):
        @pl.when(jnp.logical_not(same))
        def _():
            halves[late][-1].wait_recv()

    head_copy.wait()

    def head_rows(k):
        return head[pl.ds(pl.multiple_of(k * cols, cols), cols), :]

    def project(h, ref):
        copies = row_copies[h]
        acc = jnp.dot(ref[...], head_rows(m), preferred_element_type=F32)
        for j in range(1, n_mp, 2):
            for i in [j] if j == 1 else [j, j - 1]:
                k = flip_bits(m, i)
                copies[i].wait_recv()
                if i != 1 and i % 2 == 1:
                    copies[i - 1].start()
                acc = acc + jnp.dot(whole[k, h], head_rows(k), preferred_element_type=F32)
        return acc.astype(BF)

    s_g = alloc("s", 2)
    t_g = alloc("r", half)

    class Gather:
        def __init__(self, h):
            self.h = h
            self.t = alloc("r", parts * half)
            self.own = [
                ([self.copy(r, c, dz) for c in range(parts)], self.within(dz))
                for dz in (-1, 1)
            ]
            self.across = [self.copy(r, c, 0) for c in range(parts)]
            self.hops = {}
            for d in range(1, half):
                self.hops[d] = []
                for dz in (-1, 1):
                    origin = lax.rem(r - 2 * dz * d + 2 * n_dp, n_dp)
                    steps = [
                        (self.copy(origin, c, dz), self.copy(origin, c, 0))
                        for c in range(parts)
                    ]
                    self.hops[d].append((self.within(-dz * d), self.within(dz), steps))

        def within(self, step):
            return place + step >= 0 if step < 0 else place + step < half

        def copy(self, origin, c, dz):
            rows = ql // parts
            ref = grads.at[origin, self.h, pl.ds(c * rows, rows)]
            line = lax.div(origin, 2)
            target = lax.rem(r + 2 * dz + n_dp, n_dp) if dz else partner
            t = self.t + line * parts + c if dz else t_g + line
            return remote(ref, ref, s_g + self.h, t, dp=target)

        def start(self):
            for copies, inside in self.own:

                @pl.when(inside)
                def _(copies=copies):
                    for copy in copies:
                        copy.start()

            for copy in self.across:
                copy.start()

        def forward(self, *hops):
            for d in hops:
                for there, further, steps in self.hops[d]:

                    @pl.when(there)
                    def _(further=further, steps=steps):
                        for relay, over in steps:
                            relay.wait_recv()
                            pl.when(further)(relay.start)
                            over.start()

    slot_ids = lax.broadcasted_iota(jnp.int32, (ql, slots), 1)
    row_ids = lax.broadcasted_iota(jnp.int32, (ql, slots), 0)
    eye = slot_ids == row_ids
    from_rows = (((0,), (0,)), ((), ()))

    sel_t32 = jnp.where(rows_ref[...] == row_ids, 1.0, 0.0)
    sel_t = sel_t32.astype(BF)
    sel = jnp.transpose(sel_t32).astype(BF)
    doc = project(0, d_ref)

    def to_blocks(values, out):
        if blk % 16 == 0:
            out[...] = values.astype(BF).reshape(n_dp, blk, cols)
        else:
            flat[...] = values
            for p in range(n_dp):
                out[p] = flat[p * blk : (p + 1) * blk, :].astype(BF)

    def from_blocks(buf):
        if blk % 16 == 0:
            return buf[...].reshape(slots, cols)
        for p in range(n_dp):
            flat[p * blk : (p + 1) * blk, :] = buf[p].astype(F32)
        return flat[...].astype(BF)

    to_blocks(jnp.dot(sel, doc, preferred_element_type=F32), f_out)
    fetches = exchange(lambda peer: f_out.at[peer], lambda peer: f_in.at[r])
    f_in[r] = f_out[r]
    query = project(1, q_ref)
    hand_start(0)

    short = short_ref[...]
    named = jnp.zeros((ql, slots), F32)
    for n in range(short.shape[1]):
        named = named + jnp.where(short[:, n : n + 1] == slot_ids, 1.0, 0.0)

    col_ids = lax.broadcasted_iota(jnp.int32, (1, cols), 1)
    seg = [
        jnp.where(jnp.logical_and(col_ids >= bounds[s], col_ids < bounds[s + 1]), 1.0, 0.0)
        for s in range(n_loc)
    ]
    cut = min(256, cols)
    groups = [
        (lo, hi, [s for s in range(n_loc) if bounds[s] < hi and bounds[s + 1] > lo])
        for lo, hi in ((0, cut), (cut, cols))
        if lo < hi
    ]
    below = [jnp.where(col_ids < bounds[w + 1], 1.0, 0.0) for w in range(n_loc - 1)]
    q_prefix = jnp.concatenate([query * b.astype(BF) for b in below], axis=0)
    weight = jnp.transpose(weight_ref[...])

    came_blocks(fetches)
    fetched = from_blocks(f_in)
    against = jnp.concatenate([fetched] + [doc] * (slots // ql), axis=0)
    rhs_t = (((1,), (1,)), ((), ()))
    top = lax.dot_general(query, against, rhs_t, preferred_element_type=F32)
    pos_row = jnp.sum(jnp.where(eye, top[:, slots:], 0.0), axis=0, keepdims=True)
    ex_out[0:ql, :] = top[:, :slots]
    ex_out[ql:, :] = jnp.broadcast_to(pos_row, (8, slots))
    s1 = alloc("s", 1)
    t1 = alloc("r", n_mp - 1)
    shares = []
    for j in range(1, n_mp):
        copy = remote(ex_out, ex_in.at[m], s1, t1 + j - 1, mp=flip_bits(m, j))
        copy.start()
        shares.append(copy)
    spread(True, lambda copy: copy.start())

    def diagonal(level):
        return jnp.sum(jnp.where(eye, level, 0.0), axis=1, keepdims=True)

    def softmax(w, neg_score, pos_score):
        scale = scale_ref[w] * (1.0 / math.sqrt(bounds[w + 1]))
        neg_logit = jnp.where(named > 0.0, neg_score * scale, -1e30)
        pos_logit = pos_score * scale
        highest = jnp.maximum(jnp.max(neg_logit, axis=1, keepdims=True), pos_logit)
        neg_exp = named * jnp.exp(neg_logit - highest)
        pos_exp = jnp.exp(pos_logit - highest)
        denominator = jnp.sum(neg_exp, axis=1, keepdims=True) + pos_exp
        row_weight = weight[:, w : w + 1] * scale
        return (
            neg_exp * (row_weight / denominator),
            row_weight * (pos_exp / denominator - 1.0),
        )

    scores = lax.dot_general(q_prefix, against, rhs_t, preferred_element_type=F32)
    seg_neg = [None] * NW
    seg_pos = [None] * NW
    top_pos = diagonal(top[:, slots:])
    neg_run, pos_run = softmax(n_loc - 1, top[:, :slots], top_pos)
    seg_neg[n_loc - 1], seg_pos[n_loc - 1] = neg_run, pos_run
    for w in reversed(range(n_loc - 1)):
        level = scores[w * ql : (w + 1) * ql]
        neg_term, pos_term = softmax(w, level[:, :slots], diagonal(level[:, slots:]))
        neg_run, pos_run = neg_run + neg_term, pos_run + pos_term
        seg_neg[w], seg_pos[w] = neg_run, pos_run

    far = range(n_loc, NW)

    def inside_of(w, k):
        return jnp.where((k + 1) * cols <= bounds[w + 1], 1.0, 0.0)

    neg = {w: inside_of(w, m) * top[:, :slots] for w in far}
    pos = {w: inside_of(w, m) * top_pos for w in far}
    for j in range(1, n_mp):
        k = flip_bits(m, j)
        shares[j - 1].wait_recv()
        share = ex_in[k]
        other_neg = share[0:ql]
        other_pos = diagonal(jnp.broadcast_to(share[ql : ql + 1], (ql, slots)))
        for w in far:
            neg[w] = neg[w] + inside_of(w, k) * other_neg
            pos[w] = pos[w] + inside_of(w, k) * other_pos

    neg_run = jnp.zeros((ql, slots), F32)
    pos_run = jnp.zeros((ql, 1), F32)
    for w in reversed(far):
        neg_term, pos_term = softmax(w, neg[w], pos[w])
        neg_run, pos_run = neg_run + neg_term, pos_run + pos_term
        seg_neg[w], seg_pos[w] = neg_run, pos_run

    def local(values):
        low = [value + values[n_loc] for value in values[:n_loc]]
        mine = values[NW - 1]
        for s in reversed(range(n_loc, NW - 1)):
            mine = jnp.where((m + 1) * cols <= bounds[s + 1], values[s], mine)
        return [jnp.where(m == 0, low[0], mine)] + low[1:]

    columns = local(seg_pos)
    pos_cols = jnp.broadcast_to(columns[0], (ql, cols))
    for s in range(1, n_loc):
        here = jnp.logical_and(col_ids >= bounds[s], m == 0)
        pos_cols = jnp.where(here, columns[s], pos_cols)
    coef[...] = jnp.concatenate(local(seg_neg), axis=0).astype(BF)

    def part(s, n):
        return coef[s * ql : (s + n) * ql, :]

    @pl.when(m != 0)
    def _():
        term = lax.dot_general(part(0, 1), query, from_rows, preferred_element_type=F32)
        to_blocks(term, r_out)

    @pl.when(m == 0)
    def _():
        pieces = []
        for lo, hi, segs in groups:
            masked = [query[:, lo:hi] * seg[s][:, lo:hi].astype(BF) for s in segs]
            pieces.append(
                lax.dot_general(
                    part(segs[0], len(segs)),
                    jnp.concatenate(masked, axis=0),
                    from_rows,
                    preferred_element_type=F32,
                )
            )
        to_blocks(jnp.concatenate(pieces, axis=1), r_out)

    returns = exchange(lambda peer: r_out.at[peer], lambda peer: r_in.at[r])
    r_in[r] = r_out[r]

    @pl.when(m != 0)
    def _():
        term = jnp.dot(part(0, 1), fetched, preferred_element_type=F32)
        grads[r, 1] = (term + pos_cols * doc.astype(F32)).astype(BF)

    @pl.when(m == 0)
    def _():
        pieces = []
        for lo, hi, segs in groups:
            levels = jnp.dot(
                part(segs[0], len(segs)), fetched[:, lo:hi], preferred_element_type=F32
            )
            piece = levels[0:ql] * seg[segs[0]][:, lo:hi]
            for i in range(1, len(segs)):
                piece = piece + levels[i * ql : (i + 1) * ql] * seg[segs[i]][:, lo:hi]
            pieces.append(piece)
        term = jnp.concatenate(pieces, axis=1)
        grads[r, 1] = (term + pos_cols * doc.astype(F32)).astype(BF)

    gather_q = Gather(1)
    gather_q.start()

    s_p = alloc("s", 1)
    t_p = alloc("r", 2)

    def partial_start(h):
        value = grads[r, h]
        for j in [*range(2, n_mp), 1]:
            k = flip_bits(m, j)
            term = lax.dot_general(value, head_rows(k), rhs_t, preferred_element_type=F32)
            part_out[h, j - 1] = term.astype(BF)
            remote(part_out.at[h, j - 1], part_in.at[h, j - 1], s_p, t_p + h, mp=k).start()
        return lax.dot_general(value, head_rows(m), rhs_t, preferred_element_type=F32)

    def partial_end(h, mine):
        came_rows(t_p + h, (n_mp - 1) * ql)
        for j in range(1, n_mp):
            mine = mine + part_in[h, j - 1].astype(F32)
        return mine.astype(BF)

    part_q = partial_start(1)
    hand_pass(0)
    hand_start(1)
    came_blocks(returns)
    doc_back = jnp.dot(sel_t, from_blocks(r_in), preferred_element_type=F32)
    grads[r, 0] = (doc_back + pos_cols * query.astype(F32)).astype(BF)
    gather_d = Gather(0)
    gather_d.start()
    gather_q.forward(1)
    part_d = partial_start(0)
    gather_q.forward(*range(2, half - 1))
    gather_d.forward(1)
    gather_q.forward(*range(max(half - 1, 2), half))
    gather_d.forward(*range(2, half - 1))
    hand_pass(1)
    qg_ref[...] = partial_end(1, part_q)
    hand_end(0)
    hand_end(1)
    gather_d.forward(*range(max(half - 1, 2), half))
    dg_ref[...] = partial_end(0, part_d)
    for k in range(half):
        line = lax.rem(place + k, half)
        came_rows(t_g + line, 2 * ql)
        both = jnp.concatenate([rows_t[0, line], rows_t[1, line]], axis=1)
        term = jnp.dot(
            both,
            grads[pl.ds(line * 2, 2)].reshape(4 * ql, cols),
            preferred_element_type=F32,
        )
        if k == 0:
            hg_ref[...] = term
        else:
            hg_ref[...] += term

    inner = jnp.logical_and(place > 0, place < half - 1)

    @pl.when(inner)
    def _():
        for h in (0, 1):
            sent_rows(s_g + h, ql * (2 * half + 1))

    @pl.when(jnp.logical_not(inner))
    def _():
        for h in (0, 1):
            sent_rows(s_g + h, ql * (half + 1))

    sent_rows(s0, 2 * (n_mp - 1) * ql)
    sent_blocks(fetches)
    sent_blocks(returns)
    sent_rows(s_p, 2 * (n_mp - 1) * ql)
    others = ex_in.at[pl.ds(0, n_mp - 1)]
    remote(others, others, s1, 0, dp=partner).wait_send()
    spread(False, lambda copy: copy.wait_send())
    spread(True, lambda copy: copy.wait_send())
    half_rows = half * chunk * 2 * ql // cols

    @pl.when(m == keeper)
    def _():
        for late in (0, 1):
            sent_rows(s_f + late, n_mp // 2 * half_rows)

    @pl.when(passes)
    def _():
        for late in (0, 1):
            sent_rows(s_f + late, half_rows)


def hand_on(*refs):
    for src, dst in zip(refs[: len(refs) // 2], refs[len(refs) // 2 :]):
        dst[...] = src[...]


def solution(mesh):
    n_dp = mesh.shape["dp"]
    n_mp = mesh.shape["mp"]

    def on_device(query_rows, doc_rows, head, logit_scale, loss_grad, shortlist, send_rows):
        ql, cols = query_rows.shape
        total = n_mp * cols
        slots = send_rows.shape[1]
        blk = slots // n_dp
        chunk = total // n_dp
        n_loc = local_segments(width_bounds(total), cols)
        n_send = 9 + n_dp // n_mp
        n_recv = 3 * (n_mp - 1) + 8 + n_dp // 2 + PARTS * n_dp
        vmem = pl.BlockSpec(memory_space=pltpu.VMEM)
        shapes = (
            jax.ShapeDtypeStruct((ql, cols), BF),
            jax.ShapeDtypeStruct((ql, cols), BF),
            jax.ShapeDtypeStruct((chunk, cols), F32),
        )
        found = pl.pallas_call(
            functools.partial(kernel, n_dp, n_mp),
            out_shape=shapes,
            in_specs=[pl.BlockSpec(memory_space=pltpu.HBM)] * 7,
            out_specs=(vmem, vmem, vmem),
            scratch_shapes=[
                pltpu.VMEM((ql, cols), BF),
                pltpu.VMEM((ql, cols), BF),
                pltpu.SMEM(logit_scale.shape, F32),
                pltpu.VMEM(loss_grad.shape[::-1], F32),
                pltpu.VMEM(shortlist.shape, jnp.int32),
                pltpu.VMEM(send_rows.shape, jnp.int32),
                pltpu.VMEM((total, cols), BF),
                pltpu.VMEM((n_mp, 2, ql, cols), BF),
                pltpu.VMEM((cols, 2 * ql), BF),
                pltpu.VMEM((2, n_dp // 2, chunk, 2 * ql), BF),
                pltpu.VMEM((n_dp, blk, cols), BF),
                pltpu.VMEM((n_dp, blk, cols), BF),
                pltpu.VMEM((ql + 8, slots), F32),
                pltpu.VMEM((n_mp, ql + 8, slots), F32),
                pltpu.VMEM((n_loc * ql, slots), BF),
                pltpu.VMEM((n_dp, blk, cols), BF),
                pltpu.VMEM((n_dp, blk, cols), BF),
                pltpu.VMEM((n_dp, 2, ql, cols), BF),
                pltpu.VMEM((2, n_mp - 1, ql, cols), BF),
                pltpu.VMEM((2, n_mp - 1, ql, cols), BF),
                pltpu.VMEM((slots, cols), F32),
                pltpu.SemaphoreType.DMA((n_send,)),
                pltpu.SemaphoreType.DMA((n_recv,)),
                pltpu.SemaphoreType.DMA((8,)),
            ],
            compiler_params=pltpu.CompilerParams(
                collective_id=0, has_side_effects=True, vmem_limit_bytes=48 << 20
            ),
        )(
            *[
                pltpu.with_memory_space_constraint(x, pltpu.HBM)
                for x in (
                    query_rows,
                    doc_rows,
                    head,
                    logit_scale,
                    loss_grad.T,
                    shortlist,
                    send_rows,
                )
            ]
        )
        return pl.pallas_call(
            hand_on,
            out_shape=shapes,
            in_specs=[vmem] * 3,
            out_specs=(vmem,) * 3,
            compiler_params=pltpu.CompilerParams(vmem_limit_bytes=8 << 20),
        )(*found)

    return jax.shard_map(
        on_device,
        mesh=mesh,
        in_specs=(
            P("dp", "mp"),
            P("dp", "mp"),
            P(None, "mp"),
            P(),
            P("dp", None),
            P("dp", None),
            P("dp", None),
        ),
        out_specs=(P("dp", "mp"), P("dp", "mp"), P("dp", "mp")),
        check_vma=False,
    )
```

```python
import functools
import math

import jax
import jax.numpy as jnp
from jax import lax
from jax.experimental import pallas as pl
from jax.experimental.pallas import tpu as pltpu
from jax.sharding import PartitionSpec as P

NW = 7
PARTS = 2
MESH = pl.DeviceIdType.MESH
BF = jnp.bfloat16
F32 = jnp.float32


def width_bounds(feature_total):
    return [0] + [feature_total // 2 ** (NW - 1 - level) for level in range(NW)]


def local_segments(bounds, cols):
    return sum(bound <= cols for bound in bounds[1:])


def flip_bits(value, mask):
    bit = 1
    while bit <= mask:
        if mask & bit:
            value = value + bit - 2 * bit * lax.rem(lax.div(value, bit), 2)
        bit *= 2
    return value


def kernel(
    n_dp,
    n_mp,
    q_hbm,
    d_hbm,
    head_hbm,
    scale_hbm,
    weight_hbm,
    short_hbm,
    rows_hbm,
    qg_ref,
    dg_ref,
    hg_ref,
    q_ref,
    d_ref,
    scale_ref,
    weight_ref,
    short_ref,
    rows_ref,
    head,
    whole,
    own_t,
    rows_t,
    f_out,
    f_in,
    ex_out,
    ex_in,
    coef,
    r_out,
    r_in,
    grads,
    part_out,
    part_in,
    flat,
    ssem,
    rsem,
    lsem,
):
    ql, cols = q_ref.shape
    total = n_mp * cols
    slots = rows_ref.shape[1]
    blk = slots // n_dp
    chunk = total // n_dp
    per_mp = n_dp // n_mp
    half = n_dp // 2
    bounds = width_bounds(total)
    n_loc = local_segments(bounds, cols)
    r = lax.axis_index("dp")
    m = lax.axis_index("mp")
    partner = flip_bits(r, 1)

    counts = {}

    def alloc(kind, n):
        start = counts.get(kind, 0)
        counts[kind] = start + n
        return start

    def remote(src, dst, s, t, **where):
        return pltpu.make_async_remote_copy(
            src_ref=src,
            dst_ref=dst,
            send_sem=ssem.at[s],
            recv_sem=rsem.at[t],
            device_id=where,
            device_id_type=MESH,
        )

    loads = [
        pltpu.make_async_copy(src, dst, lsem.at[2 + i])
        for i, (src, dst) in enumerate(
            [
                (d_hbm, d_ref),
                (q_hbm, q_ref),
                (rows_hbm, rows_ref),
                (short_hbm, short_ref),
                (weight_hbm, weight_ref),
                (scale_hbm, scale_ref),
            ]
        )
    ]
    for copy in loads:
        copy.start()
    head_copy = pltpu.make_async_copy(head_hbm, head, lsem.at[0])
    head_copy.start()
    barrier = pltpu.get_barrier_semaphore()
    for j in range(1, n_mp):
        pl.semaphore_signal(
            barrier, inc=1, device_id={"mp": flip_bits(m, j)}, device_id_type=MESH
        )
    for k in range(1, n_dp):
        pl.semaphore_signal(
            barrier, inc=1, device_id={"dp": lax.rem(r + k, n_dp)}, device_id_type=MESH
        )
    for copy in loads:
        copy.wait()
    pl.semaphore_wait(barrier, n_mp - 1 + n_dp - 1)

    parts = PARTS

    def sent_rows(s, n):
        ref = head.at[pl.ds(0, n)]
        remote(ref, ref, s, 0, dp=partner).wait_send()

    def came_rows(t, n):
        ref = head.at[pl.ds(0, n)]
        remote(ref, ref, 0, t, dp=partner).wait_recv()

    def sent_blocks(pair):
        ref = f_in.at[pl.ds(0, n_dp - 1)]
        remote(ref, ref, *pair, dp=partner).wait_send()

    def came_blocks(pair):
        ref = f_in.at[pl.ds(0, n_dp - 1)]
        remote(ref, ref, *pair, dp=partner).wait_recv()

    s0 = alloc("s", 1)
    t0 = alloc("r", 2 * (n_mp - 1))
    row_copies = []
    for h, ref in enumerate((d_ref, q_ref)):
        base = h * (n_mp - 1) - 1
        copies = {}
        for j in [*range(3, n_mp, 2), 1]:
            copies[j] = remote(
                ref, whole.at[m, h], s0, t0 + base + j, mp=flip_bits(m, j)
            )
            copies[j].start()
        for j in range(3, n_mp, 2):
            k = flip_bits(m, j)
            copies[j - 1] = remote(
                whole.at[k, h],
                whole.at[k, h],
                s0,
                t0 + base + j - 1,
                mp=flip_bits(m, 1),
            )
        row_copies.append(copies)

    def exchange(out, into):
        s = alloc("s", 1)
        t = alloc("r", 1)
        for k in range(1, n_dp):
            peer = lax.rem(r + k, n_dp)
            remote(out(peer), into(peer), s, t, dp=peer).start()
        return s, t

    own = jnp.concatenate([d_ref[...], q_ref[...]], axis=0)
    own_t[...] = jnp.transpose(own)
    s_t = alloc("s", per_mp)
    t_t = alloc("r", 2)
    place = lax.div(r, 2)
    side = lax.rem(r, 2)
    keeper = lax.div(r, per_mp)

    def spread(late, step):
        for i in range(per_mp // 2):
            c = 2 * i + (1 - side if late else side)
            target = m * per_mp + c
            copy = remote(
                own_t.at[pl.ds(pl.multiple_of(c * chunk, 16), chunk)],
                rows_t.at[side, place],
                s_t + 2 * i + int(late),
                t_t + int(late),
                dp=target,
            )
            if late:
                step(copy)
            else:
                pl.when(target != r)(functools.partial(step, copy))

    spread(False, lambda copy: copy.start())

    @pl.when(m == keeper)
    def _():
        c = lax.rem(r, per_mp)
        rows_t[side, place] = own_t[pl.ds(pl.multiple_of(c * chunk, 16), chunk), :]

    s_f = alloc("s", 2)
    t_f = alloc("r", 2)
    same = lax.rem(m, 2) == lax.rem(keeper, 2)
    passes = jnp.logical_and(same, m != keeper)

    def hand_over(late):
        ref = rows_t.at[1 - side if late else side]
        return [
            remote(ref, ref, s_f + int(late), t_f + int(late), mp=flip_bits(m, j))
            for j in [*range(2, n_mp, 2), 1]
        ]

    halves = [hand_over(False), hand_over(True)]

    def hand_start(late):
        @pl.when(m == keeper)
        def _():
            n = half if late else half - 1
            came_rows(t_t + int(late), n * chunk * 2 * ql // cols)
            for copy in halves[late]:
                copy.start()

    def hand_pass(late):
        @pl.when(passes)
        def _():
            halves[late][-1].wait_recv()
            halves[late][-1].start()

    def hand_end(late):
        @pl.when(jnp.logical_not(same))
        def _():
            halves[late][-1].wait_recv()

    head_copy.wait()

    def head_rows(k):
        return head[pl.ds(pl.multiple_of(k * cols, cols), cols), :]

    def project(h, ref):
        copies = row_copies[h]
        acc = jnp.dot(ref[...], head_rows(m), preferred_element_type=F32)
        for j in range(1, n_mp, 2):
            for i in [j] if j == 1 else [j, j - 1]:
                k = flip_bits(m, i)
                copies[i].wait_recv()
                if i != 1 and i % 2 == 1:
                    copies[i - 1].start()
                acc = acc + jnp.dot(whole[k, h], head_rows(k), preferred_element_type=F32)
        return acc.astype(BF)

    s_g = alloc("s", 2)
    t_g = alloc("r", half)

    class Gather:
        def __init__(self, h):
            self.h = h
            self.t = alloc("r", parts * half)
            self.own = [
                ([self.copy(r, c, dz) for c in range(parts)], self.within(dz))
                for dz in (-1, 1)
            ]
            self.across = [self.copy(r, c, 0) for c in range(parts)]
            self.hops = {}
            for d in range(1, half):
                self.hops[d] = []
                for dz in (-1, 1):
                    origin = lax.rem(r - 2 * dz * d + 2 * n_dp, n_dp)
                    steps = [
                        (self.copy(origin, c, dz), self.copy(origin, c, 0))
                        for c in range(parts)
                    ]
                    self.hops[d].append((self.within(-dz * d), self.within(dz), steps))

        def within(self, step):
            return place + step >= 0 if step < 0 else place + step < half

        def copy(self, origin, c, dz):
            rows = ql // parts
            ref = grads.at[origin, self.h, pl.ds(c * rows, rows)]
            line = lax.div(origin, 2)
            target = lax.rem(r + 2 * dz + n_dp, n_dp) if dz else partner
            t = self.t + line * parts + c if dz else t_g + line
            return remote(ref, ref, s_g + self.h, t, dp=target)

        def start(self):
            for copies, inside in self.own:

                @pl.when(inside)
                def _(copies=copies):
                    for copy in copies:
                        copy.start()

            for copy in self.across:
                copy.start()

        def forward(self, *hops):
            for d in hops:
                for there, further, steps in self.hops[d]:

                    @pl.when(there)
                    def _(further=further, steps=steps):
                        for relay, over in steps:
                            relay.wait_recv()
                            pl.when(further)(relay.start)
                            over.start()

    slot_ids = lax.broadcasted_iota(jnp.int32, (ql, slots), 1)
    row_ids = lax.broadcasted_iota(jnp.int32, (ql, slots), 0)
    eye = slot_ids == row_ids
    from_rows = (((0,), (0,)), ((), ()))

    sel_t32 = jnp.where(rows_ref[...] == row_ids, 1.0, 0.0)
    sel_t = sel_t32.astype(BF)
    sel = jnp.transpose(sel_t32).astype(BF)
    doc = project(0, d_ref)

    def to_blocks(values, out):
        if blk % 16 == 0:
            out[...] = values.astype(BF).reshape(n_dp, blk, cols)
        else:
            flat[...] = values
            for p in range(n_dp):
                out[p] = flat[p * blk : (p + 1) * blk, :].astype(BF)

    def from_blocks(buf):
        if blk % 16 == 0:
            return buf[...].reshape(slots, cols)
        for p in range(n_dp):
            flat[p * blk : (p + 1) * blk, :] = buf[p].astype(F32)
        return flat[...].astype(BF)

    to_blocks(jnp.dot(sel, doc, preferred_element_type=F32), f_out)
    fetches = exchange(lambda peer: f_out.at[peer], lambda peer: f_in.at[r])
    f_in[r] = f_out[r]
    query = project(1, q_ref)
    hand_start(0)

    short = short_ref[...]
    named = jnp.zeros((ql, slots), F32)
    for n in range(short.shape[1]):
        named = named + jnp.where(short[:, n : n + 1] == slot_ids, 1.0, 0.0)

    col_ids = lax.broadcasted_iota(jnp.int32, (1, cols), 1)
    seg = [
        jnp.where(jnp.logical_and(col_ids >= bounds[s], col_ids < bounds[s + 1]), 1.0, 0.0)
        for s in range(n_loc)
    ]
    cut = min(256, cols)
    groups = [
        (lo, hi, [s for s in range(n_loc) if bounds[s] < hi and bounds[s + 1] > lo])
        for lo, hi in ((0, cut), (cut, cols))
        if lo < hi
    ]
    below = [jnp.where(col_ids < bounds[w + 1], 1.0, 0.0) for w in range(n_loc - 1)]
    q_prefix = jnp.concatenate([query * b.astype(BF) for b in below], axis=0)
    weight = jnp.transpose(weight_ref[...])

    came_blocks(fetches)
    fetched = from_blocks(f_in)
    against = jnp.concatenate([fetched] + [doc] * (slots // ql), axis=0)
    rhs_t = (((1,), (1,)), ((), ()))
    top = lax.dot_general(query, against, rhs_t, preferred_element_type=F32)
    pos_row = jnp.sum(jnp.where(eye, top[:, slots:], 0.0), axis=0, keepdims=True)
    ex_out[0:ql, :] = top[:, :slots]
    ex_out[ql:, :] = jnp.broadcast_to(pos_row, (8, slots))
    s1 = alloc("s", 1)
    t1 = alloc("r", n_mp - 1)
    shares = []
    for j in range(1, n_mp):
        copy = remote(ex_out, ex_in.at[m], s1, t1 + j - 1, mp=flip_bits(m, j))
        copy.start()
        shares.append(copy)
    spread(True, lambda copy: copy.start())

    def diagonal(level):
        return jnp.sum(jnp.where(eye, level, 0.0), axis=1, keepdims=True)

    def softmax(w, neg_score, pos_score):
        scale = scale_ref[w] * (1.0 / math.sqrt(bounds[w + 1]))
        neg_logit = jnp.where(named > 0.0, neg_score * scale, -1e30)
        pos_logit = pos_score * scale
        highest = jnp.maximum(jnp.max(neg_logit, axis=1, keepdims=True), pos_logit)
        neg_exp = named * jnp.exp(neg_logit - highest)
        pos_exp = jnp.exp(pos_logit - highest)
        denominator = jnp.sum(neg_exp, axis=1, keepdims=True) + pos_exp
        row_weight = weight[:, w : w + 1] * scale
        return (
            neg_exp * (row_weight / denominator),
            row_weight * (pos_exp / denominator - 1.0),
        )

    scores = lax.dot_general(q_prefix, against, rhs_t, preferred_element_type=F32)
    seg_neg = [None] * NW
    seg_pos = [None] * NW
    top_pos = diagonal(top[:, slots:])
    neg_run, pos_run = softmax(n_loc - 1, top[:, :slots], top_pos)
    seg_neg[n_loc - 1], seg_pos[n_loc - 1] = neg_run, pos_run
    for w in reversed(range(n_loc - 1)):
        level = scores[w * ql : (w + 1) * ql]
        neg_term, pos_term = softmax(w, level[:, :slots], diagonal(level[:, slots:]))
        neg_run, pos_run = neg_run + neg_term, pos_run + pos_term
        seg_neg[w], seg_pos[w] = neg_run, pos_run

    far = range(n_loc, NW)

    def inside_of(w, k):
        return jnp.where((k + 1) * cols <= bounds[w + 1], 1.0, 0.0)

    neg = {w: inside_of(w, m) * top[:, :slots] for w in far}
    pos = {w: inside_of(w, m) * top_pos for w in far}
    for j in range(1, n_mp):
        k = flip_bits(m, j)
        shares[j - 1].wait_recv()
        share = ex_in[k]
        other_neg = share[0:ql]
        other_pos = diagonal(jnp.broadcast_to(share[ql : ql + 1], (ql, slots)))
        for w in far:
            neg[w] = neg[w] + inside_of(w, k) * other_neg
            pos[w] = pos[w] + inside_of(w, k) * other_pos

    neg_run = jnp.zeros((ql, slots), F32)
    pos_run = jnp.zeros((ql, 1), F32)
    for w in reversed(far):
        neg_term, pos_term = softmax(w, neg[w], pos[w])
        neg_run, pos_run = neg_run + neg_term, pos_run + pos_term
        seg_neg[w], seg_pos[w] = neg_run, pos_run

    def local(values):
        low = [value + values[n_loc] for value in values[:n_loc]]
        mine = values[NW - 1]
        for s in reversed(range(n_loc, NW - 1)):
            mine = jnp.where((m + 1) * cols <= bounds[s + 1], values[s], mine)
        return [jnp.where(m == 0, low[0], mine)] + low[1:]

    columns = local(seg_pos)
    pos_cols = jnp.broadcast_to(columns[0], (ql, cols))
    for s in range(1, n_loc):
        here = jnp.logical_and(col_ids >= bounds[s], m == 0)
        pos_cols = jnp.where(here, columns[s], pos_cols)
    coef[...] = jnp.concatenate(local(seg_neg), axis=0).astype(BF)

    def part(s, n):
        return coef[s * ql : (s + n) * ql, :]

    @pl.when(m != 0)
    def _():
        term = lax.dot_general(part(0, 1), query, from_rows, preferred_element_type=F32)
        to_blocks(term, r_out)

    @pl.when(m == 0)
    def _():
        pieces = []
        for lo, hi, segs in groups:
            masked = [query[:, lo:hi] * seg[s][:, lo:hi].astype(BF) for s in segs]
            pieces.append(
                lax.dot_general(
                    part(segs[0], len(segs)),
                    jnp.concatenate(masked, axis=0),
                    from_rows,
                    preferred_element_type=F32,
                )
            )
        to_blocks(jnp.concatenate(pieces, axis=1), r_out)

    returns = exchange(lambda peer: r_out.at[peer], lambda peer: r_in.at[r])
    r_in[r] = r_out[r]

    @pl.when(m != 0)
    def _():
        term = jnp.dot(part(0, 1), fetched, preferred_element_type=F32)
        grads[r, 1] = (term + pos_cols * doc.astype(F32)).astype(BF)

    @pl.when(m == 0)
    def _():
        pieces = []
        for lo, hi, segs in groups:
            levels = jnp.dot(
                part(segs[0], len(segs)), fetched[:, lo:hi], preferred_element_type=F32
            )
            piece = levels[0:ql] * seg[segs[0]][:, lo:hi]
            for i in range(1, len(segs)):
                piece = piece + levels[i * ql : (i + 1) * ql] * seg[segs[i]][:, lo:hi]
            pieces.append(piece)
        term = jnp.concatenate(pieces, axis=1)
        grads[r, 1] = (term + pos_cols * doc.astype(F32)).astype(BF)

    gather_q = Gather(1)
    gather_q.start()

    s_p = alloc("s", 1)
    t_p = alloc("r", 2)

    def partial_start(h):
        value = grads[r, h]
        for j in [*range(2, n_mp), 1]:
            k = flip_bits(m, j)
            term = lax.dot_general(value, head_rows(k), rhs_t, preferred_element_type=F32)
            part_out[h, j - 1] = term.astype(BF)
            remote(part_out.at[h, j - 1], part_in.at[h, j - 1], s_p, t_p + h, mp=k).start()
        return lax.dot_general(value, head_rows(m), rhs_t, preferred_element_type=F32)

    def partial_end(h, mine):
        came_rows(t_p + h, (n_mp - 1) * ql)
        for j in range(1, n_mp):
            mine = mine + part_in[h, j - 1].astype(F32)
        return mine.astype(BF)

    part_q = partial_start(1)
    hand_pass(0)
    hand_start(1)
    came_blocks(returns)
    doc_back = jnp.dot(sel_t, from_blocks(r_in), preferred_element_type=F32)
    grads[r, 0] = (doc_back + pos_cols * query.astype(F32)).astype(BF)
    gather_d = Gather(0)
    gather_d.start()
    gather_q.forward(1)
    part_d = partial_start(0)
    gather_d.forward(1)
    gather_q.forward(*range(2, half - 1))
    gather_d.forward(*range(2, half - 1))
    gather_q.forward(*range(max(half - 1, 2), half))
    hand_pass(1)
    qg_ref[...] = partial_end(1, part_q)
    hand_end(0)
    hand_end(1)
    gather_d.forward(*range(max(half - 1, 2), half))
    dg_ref[...] = partial_end(0, part_d)
    for k in range(half):
        line = lax.rem(place + k, half)
        came_rows(t_g + line, 2 * ql)
        both = jnp.concatenate([rows_t[0, line], rows_t[1, line]], axis=1)
        term = jnp.dot(
            both,
            grads[pl.ds(line * 2, 2)].reshape(4 * ql, cols),
            preferred_element_type=F32,
        )
        if k == 0:
            hg_ref[...] = term
        else:
            hg_ref[...] += term

    inner = jnp.logical_and(place > 0, place < half - 1)

    @pl.when(inner)
    def _():
        for h in (0, 1):
            sent_rows(s_g + h, ql * (2 * half + 1))

    @pl.when(jnp.logical_not(inner))
    def _():
        for h in (0, 1):
            sent_rows(s_g + h, ql * (half + 1))

    sent_rows(s0, 2 * (n_mp - 1) * ql)
    sent_blocks(fetches)
    sent_blocks(returns)
    sent_rows(s_p, 2 * (n_mp - 1) * ql)
    others = ex_in.at[pl.ds(0, n_mp - 1)]
    remote(others, others, s1, 0, dp=partner).wait_send()
    spread(False, lambda copy: copy.wait_send())
    spread(True, lambda copy: copy.wait_send())
    half_rows = half * chunk * 2 * ql // cols

    @pl.when(m == keeper)
    def _():
        for late in (0, 1):
            sent_rows(s_f + late, n_mp // 2 * half_rows)

    @pl.when(passes)
    def _():
        for late in (0, 1):
            sent_rows(s_f + late, half_rows)


def hand_on(*refs):
    for src, dst in zip(refs[: len(refs) // 2], refs[len(refs) // 2 :]):
        dst[...] = src[...]


def solution(mesh):
    n_dp = mesh.shape["dp"]
    n_mp = mesh.shape["mp"]

    def on_device(query_rows, doc_rows, head, logit_scale, loss_grad, shortlist, send_rows):
        ql, cols = query_rows.shape
        total = n_mp * cols
        slots = send_rows.shape[1]
        blk = slots // n_dp
        chunk = total // n_dp
        n_loc = local_segments(width_bounds(total), cols)
        n_send = 9 + n_dp // n_mp
        n_recv = 3 * (n_mp - 1) + 8 + n_dp // 2 + PARTS * n_dp
        vmem = pl.BlockSpec(memory_space=pltpu.VMEM)
        shapes = (
            jax.ShapeDtypeStruct((ql, cols), BF),
            jax.ShapeDtypeStruct((ql, cols), BF),
            jax.ShapeDtypeStruct((chunk, cols), F32),
        )
        found = pl.pallas_call(
            functools.partial(kernel, n_dp, n_mp),
            out_shape=shapes,
            in_specs=[pl.BlockSpec(memory_space=pltpu.HBM)] * 7,
            out_specs=(vmem, vmem, vmem),
            scratch_shapes=[
                pltpu.VMEM((ql, cols), BF),
                pltpu.VMEM((ql, cols), BF),
                pltpu.SMEM(logit_scale.shape, F32),
                pltpu.VMEM(loss_grad.shape[::-1], F32),
                pltpu.VMEM(shortlist.shape, jnp.int32),
                pltpu.VMEM(send_rows.shape, jnp.int32),
                pltpu.VMEM((total, cols), BF),
                pltpu.VMEM((n_mp, 2, ql, cols), BF),
                pltpu.VMEM((cols, 2 * ql), BF),
                pltpu.VMEM((2, n_dp // 2, chunk, 2 * ql), BF),
                pltpu.VMEM((n_dp, blk, cols), BF),
                pltpu.VMEM((n_dp, blk, cols), BF),
                pltpu.VMEM((ql + 8, slots), F32),
                pltpu.VMEM((n_mp, ql + 8, slots), F32),
                pltpu.VMEM((n_loc * ql, slots), BF),
                pltpu.VMEM((n_dp, blk, cols), BF),
                pltpu.VMEM((n_dp, blk, cols), BF),
                pltpu.VMEM((n_dp, 2, ql, cols), BF),
                pltpu.VMEM((2, n_mp - 1, ql, cols), BF),
                pltpu.VMEM((2, n_mp - 1, ql, cols), BF),
                pltpu.VMEM((slots, cols), F32),
                pltpu.SemaphoreType.DMA((n_send,)),
                pltpu.SemaphoreType.DMA((n_recv,)),
                pltpu.SemaphoreType.DMA((8,)),
            ],
            compiler_params=pltpu.CompilerParams(
                collective_id=0, has_side_effects=True, vmem_limit_bytes=48 << 20
            ),
        )(
            *[
                pltpu.with_memory_space_constraint(x, pltpu.HBM)
                for x in (
                    query_rows,
                    doc_rows,
                    head,
                    logit_scale,
                    loss_grad.T,
                    shortlist,
                    send_rows,
                )
            ]
        )
        return pl.pallas_call(
            hand_on,
            out_shape=shapes,
            in_specs=[vmem] * 3,
            out_specs=(vmem,) * 3,
            compiler_params=pltpu.CompilerParams(vmem_limit_bytes=8 << 20),
        )(*found)

    return jax.shard_map(
        on_device,
        mesh=mesh,
        in_specs=(
            P("dp", "mp"),
            P("dp", "mp"),
            P(None, "mp"),
            P(),
            P("dp", None),
            P("dp", None),
            P("dp", None),
        ),
        out_specs=(P("dp", "mp"), P("dp", "mp"), P("dp", "mp")),
        check_vma=False,
    )
```

```python
import functools
import math

import jax
import jax.numpy as jnp
from jax import lax
from jax.experimental import pallas as pl
from jax.experimental.pallas import tpu as pltpu
from jax.sharding import PartitionSpec as P

NW = 7
PARTS = 2
MESH = pl.DeviceIdType.MESH
BF = jnp.bfloat16
F32 = jnp.float32


def width_bounds(feature_total):
    return [0] + [feature_total // 2 ** (NW - 1 - level) for level in range(NW)]


def local_segments(bounds, cols):
    return sum(bound <= cols for bound in bounds[1:])


def flip_bits(value, mask):
    bit = 1
    while bit <= mask:
        if mask & bit:
            value = value + bit - 2 * bit * lax.rem(lax.div(value, bit), 2)
        bit *= 2
    return value


def kernel(
    n_dp,
    n_mp,
    q_hbm,
    d_hbm,
    head_hbm,
    scale_hbm,
    weight_hbm,
    short_hbm,
    rows_hbm,
    qg_ref,
    dg_ref,
    hg_ref,
    q_ref,
    d_ref,
    scale_ref,
    weight_ref,
    short_ref,
    rows_ref,
    head,
    whole,
    own_t,
    rows_t,
    f_out,
    f_in,
    ex_out,
    ex_in,
    coef,
    r_out,
    r_in,
    grads,
    part_out,
    part_in,
    flat,
    ssem,
    rsem,
    lsem,
):
    ql, cols = q_ref.shape
    total = n_mp * cols
    slots = rows_ref.shape[1]
    blk = slots // n_dp
    chunk = total // n_dp
    per_mp = n_dp // n_mp
    half = n_dp // 2
    bounds = width_bounds(total)
    n_loc = local_segments(bounds, cols)
    r = lax.axis_index("dp")
    m = lax.axis_index("mp")
    partner = flip_bits(r, 1)

    counts = {}

    def alloc(kind, n):
        start = counts.get(kind, 0)
        counts[kind] = start + n
        return start

    def remote(src, dst, s, t, **where):
        return pltpu.make_async_remote_copy(
            src_ref=src,
            dst_ref=dst,
            send_sem=ssem.at[s],
            recv_sem=rsem.at[t],
            device_id=where,
            device_id_type=MESH,
        )

    loads = [
        pltpu.make_async_copy(src, dst, lsem.at[2 + i])
        for i, (src, dst) in enumerate(
            [
                (d_hbm, d_ref),
                (q_hbm, q_ref),
                (rows_hbm, rows_ref),
                (short_hbm, short_ref),
                (weight_hbm, weight_ref),
                (scale_hbm, scale_ref),
            ]
        )
    ]
    for copy in loads:
        copy.start()
    head_copy = pltpu.make_async_copy(head_hbm, head, lsem.at[0])
    head_copy.start()
    barrier = pltpu.get_barrier_semaphore()
    for j in range(1, n_mp):
        pl.semaphore_signal(
            barrier, inc=1, device_id={"mp": flip_bits(m, j)}, device_id_type=MESH
        )
    for k in range(1, n_dp):
        pl.semaphore_signal(
            barrier, inc=1, device_id={"dp": lax.rem(r + k, n_dp)}, device_id_type=MESH
        )
    for copy in loads:
        copy.wait()
    pl.semaphore_wait(barrier, n_mp - 1 + n_dp - 1)

    parts = PARTS

    def sent_rows(s, n):
        ref = head.at[pl.ds(0, n)]
        remote(ref, ref, s, 0, dp=partner).wait_send()

    def came_rows(t, n):
        ref = head.at[pl.ds(0, n)]
        remote(ref, ref, 0, t, dp=partner).wait_recv()

    def sent_blocks(pair):
        ref = f_in.at[pl.ds(0, n_dp - 1)]
        remote(ref, ref, *pair, dp=partner).wait_send()

    def came_blocks(pair):
        ref = f_in.at[pl.ds(0, n_dp - 1)]
        remote(ref, ref, *pair, dp=partner).wait_recv()

    s0 = alloc("s", 1)
    t0 = alloc("r", 2 * (n_mp - 1))
    row_copies = []
    for h, ref in enumerate((d_ref, q_ref)):
        base = h * (n_mp - 1) - 1
        copies = {}
        for j in [*range(3, n_mp, 2), 1]:
            copies[j] = remote(
                ref, whole.at[m, h], s0, t0 + base + j, mp=flip_bits(m, j)
            )
            copies[j].start()
        for j in range(3, n_mp, 2):
            k = flip_bits(m, j)
            copies[j - 1] = remote(
                whole.at[k, h],
                whole.at[k, h],
                s0,
                t0 + base + j - 1,
                mp=flip_bits(m, 1),
            )
        row_copies.append(copies)

    def exchange(out, into):
        s = alloc("s", 1)
        t = alloc("r", 1)
        for k in range(1, n_dp):
            peer = lax.rem(r + k, n_dp)
            remote(out(peer), into(peer), s, t, dp=peer).start()
        return s, t

    own = jnp.concatenate([d_ref[...], q_ref[...]], axis=0)
    own_t[...] = jnp.transpose(own)
    s_t = alloc("s", per_mp)
    t_t = alloc("r", 2)
    place = lax.div(r, 2)
    side = lax.rem(r, 2)
    keeper = lax.div(r, per_mp)

    def spread(late, step):
        for i in range(per_mp // 2):
            c = 2 * i + (1 - side if late else side)
            target = m * per_mp + c
            copy = remote(
                own_t.at[pl.ds(pl.multiple_of(c * chunk, 16), chunk)],
                rows_t.at[side, place],
                s_t + 2 * i + int(late),
                t_t + int(late),
                dp=target,
            )
            if late:
                step(copy)
            else:
                pl.when(target != r)(functools.partial(step, copy))

    spread(False, lambda copy: copy.start())

    @pl.when(m == keeper)
    def _():
        c = lax.rem(r, per_mp)
        rows_t[side, place] = own_t[pl.ds(pl.multiple_of(c * chunk, 16), chunk), :]

    s_f = alloc("s", 2)
    t_f = alloc("r", 2)
    same = lax.rem(m, 2) == lax.rem(keeper, 2)
    passes = jnp.logical_and(same, m != keeper)

    def hand_over(late):
        ref = rows_t.at[1 - side if late else side]
        return [
            remote(ref, ref, s_f + int(late), t_f + int(late), mp=flip_bits(m, j))
            for j in [*range(2, n_mp, 2), 1]
        ]

    halves = [hand_over(False), hand_over(True)]

    def hand_start(late):
        @pl.when(m == keeper)
        def _():
            n = half if late else half - 1
            came_rows(t_t + int(late), n * chunk * 2 * ql // cols)
            for copy in halves[late]:
                copy.start()

    def hand_pass(late):
        @pl.when(passes)
        def _():
            halves[late][-1].wait_recv()
            halves[late][-1].start()

    def hand_end(late):
        @pl.when(jnp.logical_not(same))
        def _():
            halves[late][-1].wait_recv()

    head_copy.wait()

    def head_rows(k):
        return head[pl.ds(pl.multiple_of(k * cols, cols), cols), :]

    def project(h, ref):
        copies = row_copies[h]
        acc = jnp.dot(ref[...], head_rows(m), preferred_element_type=F32)
        for j in range(1, n_mp, 2):
            for i in [j] if j == 1 else [j, j - 1]:
                k = flip_bits(m, i)
                copies[i].wait_recv()
                if i != 1 and i % 2 == 1:
                    copies[i - 1].start()
                acc = acc + jnp.dot(whole[k, h], head_rows(k), preferred_element_type=F32)
        return acc.astype(BF)

    s_g = alloc("s", 2)
    t_g = alloc("r", half)

    class Gather:
        def __init__(self, h):
            self.h = h
            self.t = alloc("r", parts * half)
            self.own = [
                ([self.copy(r, c, dz) for c in range(parts)], self.within(dz))
                for dz in (-1, 1)
            ]
            self.across = [self.copy(r, c, 0) for c in range(parts)]
            self.hops = {}
            for d in range(1, half):
                self.hops[d] = []
                for dz in (-1, 1):
                    origin = lax.rem(r - 2 * dz * d + 2 * n_dp, n_dp)
                    steps = [
                        (self.copy(origin, c, dz), self.copy(origin, c, 0))
                        for c in range(parts)
                    ]
                    self.hops[d].append((self.within(-dz * d), self.within(dz), steps))

        def within(self, step):
            return place + step >= 0 if step < 0 else place + step < half

        def copy(self, origin, c, dz):
            rows = ql // parts
            ref = grads.at[origin, self.h, pl.ds(c * rows, rows)]
            line = lax.div(origin, 2)
            target = lax.rem(r + 2 * dz + n_dp, n_dp) if dz else partner
            t = self.t + line * parts + c if dz else t_g + line
            return remote(ref, ref, s_g + self.h, t, dp=target)

        def start(self):
            for copies, inside in self.own:

                @pl.when(inside)
                def _(copies=copies):
                    for copy in copies:
                        copy.start()

            for copy in self.across:
                copy.start()

        def forward(self, *hops):
            for d in hops:
                for there, further, steps in self.hops[d]:

                    @pl.when(there)
                    def _(further=further, steps=steps):
                        for relay, over in steps:
                            relay.wait_recv()
                            pl.when(further)(relay.start)
                            over.start()

    slot_ids = lax.broadcasted_iota(jnp.int32, (ql, slots), 1)
    row_ids = lax.broadcasted_iota(jnp.int32, (ql, slots), 0)
    eye = slot_ids == row_ids
    from_rows = (((0,), (0,)), ((), ()))

    sel_t32 = jnp.where(rows_ref[...] == row_ids, 1.0, 0.0)
    sel_t = sel_t32.astype(BF)
    sel = jnp.transpose(sel_t32).astype(BF)
    doc = project(0, d_ref)

    def to_blocks(values, out):
        if blk % 16 == 0:
            out[...] = values.astype(BF).reshape(n_dp, blk, cols)
        else:
            flat[...] = values
            for p in range(n_dp):
                out[p] = flat[p * blk : (p + 1) * blk, :].astype(BF)

    def from_blocks(buf):
        if blk % 16 == 0:
            return buf[...].reshape(slots, cols)
        for p in range(n_dp):
            flat[p * blk : (p + 1) * blk, :] = buf[p].astype(F32)
        return flat[...].astype(BF)

    to_blocks(jnp.dot(sel, doc, preferred_element_type=F32), f_out)
    fetches = exchange(lambda peer: f_out.at[peer], lambda peer: f_in.at[r])
    f_in[r] = f_out[r]
    query = project(1, q_ref)
    hand_start(0)

    short = short_ref[...]
    named = jnp.zeros((ql, slots), F32)
    for n in range(short.shape[1]):
        named = named + jnp.where(short[:, n : n + 1] == slot_ids, 1.0, 0.0)

    col_ids = lax.broadcasted_iota(jnp.int32, (1, cols), 1)
    seg = [
        jnp.where(jnp.logical_and(col_ids >= bounds[s], col_ids < bounds[s + 1]), 1.0, 0.0)
        for s in range(n_loc)
    ]
    cut = min(256, cols)
    groups = [
        (lo, hi, [s for s in range(n_loc) if bounds[s] < hi and bounds[s + 1] > lo])
        for lo, hi in ((0, cut), (cut, cols))
        if lo < hi
    ]
    below = [jnp.where(col_ids < bounds[w + 1], 1.0, 0.0) for w in range(n_loc - 1)]
    q_prefix = jnp.concatenate([query * b.astype(BF) for b in below], axis=0)
    weight = jnp.transpose(weight_ref[...])

    came_blocks(fetches)
    fetched = from_blocks(f_in)
    against = jnp.concatenate([fetched] + [doc] * (slots // ql), axis=0)
    rhs_t = (((1,), (1,)), ((), ()))
    top = lax.dot_general(query, against, rhs_t, preferred_element_type=F32)
    pos_row = jnp.sum(jnp.where(eye, top[:, slots:], 0.0), axis=0, keepdims=True)
    ex_out[0:ql, :] = top[:, :slots]
    ex_out[ql:, :] = jnp.broadcast_to(pos_row, (8, slots))
    s1 = alloc("s", 1)
    t1 = alloc("r", n_mp - 1)
    shares = []
    for j in range(1, n_mp):
        copy = remote(ex_out, ex_in.at[m], s1, t1 + j - 1, mp=flip_bits(m, j))
        copy.start()
        shares.append(copy)
    spread(True, lambda copy: copy.start())

    def diagonal(level):
        return jnp.sum(jnp.where(eye, level, 0.0), axis=1, keepdims=True)

    def softmax(w, neg_score, pos_score):
        scale = scale_ref[w] * (1.0 / math.sqrt(bounds[w + 1]))
        neg_logit = jnp.where(named > 0.0, neg_score * scale, -1e30)
        pos_logit = pos_score * scale
        highest = jnp.maximum(jnp.max(neg_logit, axis=1, keepdims=True), pos_logit)
        neg_exp = named * jnp.exp(neg_logit - highest)
        pos_exp = jnp.exp(pos_logit - highest)
        denominator = jnp.sum(neg_exp, axis=1, keepdims=True) + pos_exp
        row_weight = weight[:, w : w + 1] * scale
        return (
            neg_exp * (row_weight / denominator),
            row_weight * (pos_exp / denominator - 1.0),
        )

    scores = lax.dot_general(q_prefix, against, rhs_t, preferred_element_type=F32)
    seg_neg = [None] * NW
    seg_pos = [None] * NW
    top_pos = diagonal(top[:, slots:])
    neg_run, pos_run = softmax(n_loc - 1, top[:, :slots], top_pos)
    seg_neg[n_loc - 1], seg_pos[n_loc - 1] = neg_run, pos_run
    for w in reversed(range(n_loc - 1)):
        level = scores[w * ql : (w + 1) * ql]
        neg_term, pos_term = softmax(w, level[:, :slots], diagonal(level[:, slots:]))
        neg_run, pos_run = neg_run + neg_term, pos_run + pos_term
        seg_neg[w], seg_pos[w] = neg_run, pos_run

    far = range(n_loc, NW)

    def inside_of(w, k):
        return jnp.where((k + 1) * cols <= bounds[w + 1], 1.0, 0.0)

    neg = {w: inside_of(w, m) * top[:, :slots] for w in far}
    pos = {w: inside_of(w, m) * top_pos for w in far}
    for j in range(1, n_mp):
        k = flip_bits(m, j)
        shares[j - 1].wait_recv()
        share = ex_in[k]
        other_neg = share[0:ql]
        other_pos = diagonal(jnp.broadcast_to(share[ql : ql + 1], (ql, slots)))
        for w in far:
            neg[w] = neg[w] + inside_of(w, k) * other_neg
            pos[w] = pos[w] + inside_of(w, k) * other_pos

    neg_run = jnp.zeros((ql, slots), F32)
    pos_run = jnp.zeros((ql, 1), F32)
    for w in reversed(far):
        neg_term, pos_term = softmax(w, neg[w], pos[w])
        neg_run, pos_run = neg_run + neg_term, pos_run + pos_term
        seg_neg[w], seg_pos[w] = neg_run, pos_run

    def local(values):
        low = [value + values[n_loc] for value in values[:n_loc]]
        mine = values[NW - 1]
        for s in reversed(range(n_loc, NW - 1)):
            mine = jnp.where((m + 1) * cols <= bounds[s + 1], values[s], mine)
        return [jnp.where(m == 0, low[0], mine)] + low[1:]

    columns = local(seg_pos)
    pos_cols = jnp.broadcast_to(columns[0], (ql, cols))
    for s in range(1, n_loc):
        here = jnp.logical_and(col_ids >= bounds[s], m == 0)
        pos_cols = jnp.where(here, columns[s], pos_cols)
    coef[...] = jnp.concatenate(local(seg_neg), axis=0).astype(BF)

    def part(s, n):
        return coef[s * ql : (s + n) * ql, :]

    @pl.when(m != 0)
    def _():
        term = lax.dot_general(part(0, 1), query, from_rows, preferred_element_type=F32)
        to_blocks(term, r_out)

    @pl.when(m == 0)
    def _():
        pieces = []
        for lo, hi, segs in groups:
            masked = [query[:, lo:hi] * seg[s][:, lo:hi].astype(BF) for s in segs]
            pieces.append(
                lax.dot_general(
                    part(segs[0], len(segs)),
                    jnp.concatenate(masked, axis=0),
                    from_rows,
                    preferred_element_type=F32,
                )
            )
        to_blocks(jnp.concatenate(pieces, axis=1), r_out)

    returns = exchange(lambda peer: r_out.at[peer], lambda peer: r_in.at[r])
    r_in[r] = r_out[r]

    @pl.when(m != 0)
    def _():
        term = jnp.dot(part(0, 1), fetched, preferred_element_type=F32)
        grads[r, 1] = (term + pos_cols * doc.astype(F32)).astype(BF)

    @pl.when(m == 0)
    def _():
        pieces = []
        for lo, hi, segs in groups:
            levels = jnp.dot(
                part(segs[0], len(segs)), fetched[:, lo:hi], preferred_element_type=F32
            )
            piece = levels[0:ql] * seg[segs[0]][:, lo:hi]
            for i in range(1, len(segs)):
                piece = piece + levels[i * ql : (i + 1) * ql] * seg[segs[i]][:, lo:hi]
            pieces.append(piece)
        term = jnp.concatenate(pieces, axis=1)
        grads[r, 1] = (term + pos_cols * doc.astype(F32)).astype(BF)

    gather_q = Gather(1)
    gather_q.start()

    s_p = alloc("s", 1)
    t_p = alloc("r", 2)

    def partial_start(h):
        value = grads[r, h]
        for j in [*range(2, n_mp), 1]:
            k = flip_bits(m, j)
            term = lax.dot_general(value, head_rows(k), rhs_t, preferred_element_type=F32)
            part_out[h, j - 1] = term.astype(BF)
            remote(part_out.at[h, j - 1], part_in.at[h, j - 1], s_p, t_p + h, mp=k).start()
        return lax.dot_general(value, head_rows(m), rhs_t, preferred_element_type=F32)

    def partial_end(h, mine):
        came_rows(t_p + h, (n_mp - 1) * ql)
        for j in range(1, n_mp):
            mine = mine + part_in[h, j - 1].astype(F32)
        return mine.astype(BF)

    part_q = partial_start(1)
    hand_pass(0)
    hand_start(1)
    came_blocks(returns)
    doc_back = jnp.dot(sel_t, from_blocks(r_in), preferred_element_type=F32)
    grads[r, 0] = (doc_back + pos_cols * query.astype(F32)).astype(BF)
    gather_d = Gather(0)
    gather_d.start()
    gather_q.forward(1)
    part_d = partial_start(0)
    gather_d.forward(1)
    gather_q.forward(*range(2, half - 1))
    gather_d.forward(*range(2, half - 1))
    gather_q.forward(*range(max(half - 1, 2), half))
    hand_pass(1)
    qg_ref[...] = partial_end(1, part_q)
    hand_end(0)
    hand_end(1)
    gather_d.forward(*range(max(half - 1, 2), half))
    dg_ref[...] = partial_end(0, part_d)
    for k in range(half):
        line = lax.rem(place + k, half)
        came_rows(t_g + line, 2 * ql)
        both = jnp.concatenate([rows_t[0, line], rows_t[1, line]], axis=1)
        term = jnp.dot(
            both,
            grads[pl.ds(line * 2, 2)].reshape(4 * ql, cols),
            preferred_element_type=F32,
        )
        if k == 0:
            hg_ref[...] = term
        else:
            hg_ref[...] += term

    inner = jnp.logical_and(place > 0, place < half - 1)

    @pl.when(inner)
    def _():
        for h in (0, 1):
            sent_rows(s_g + h, ql * (2 * half + 1))

    @pl.when(jnp.logical_not(inner))
    def _():
        for h in (0, 1):
            sent_rows(s_g + h, ql * (half + 1))

    sent_rows(s0, 2 * (n_mp - 1) * ql)
    sent_blocks(fetches)
    sent_blocks(returns)
    sent_rows(s_p, 2 * (n_mp - 1) * ql)
    others = ex_in.at[pl.ds(0, n_mp - 1)]
    remote(others, others, s1, 0, dp=partner).wait_send()
    spread(False, lambda copy: copy.wait_send())
    spread(True, lambda copy: copy.wait_send())
    half_rows = half * chunk * 2 * ql // cols

    @pl.when(m == keeper)
    def _():
        for late in (0, 1):
            sent_rows(s_f + late, n_mp // 2 * half_rows)

    @pl.when(passes)
    def _():
        for late in (0, 1):
            sent_rows(s_f + late, half_rows)


def hand_on(*refs):
    n = len(refs) // 2
    copies = [pltpu.make_async_copy(refs[i], refs[n + i], refs[-1].at[i]) for i in range(n)]
    for copy in reversed(copies):
        copy.start()
    for copy in copies:
        copy.wait()


def solution(mesh):
    n_dp = mesh.shape["dp"]
    n_mp = mesh.shape["mp"]

    def on_device(query_rows, doc_rows, head, logit_scale, loss_grad, shortlist, send_rows):
        ql, cols = query_rows.shape
        total = n_mp * cols
        slots = send_rows.shape[1]
        blk = slots // n_dp
        chunk = total // n_dp
        n_loc = local_segments(width_bounds(total), cols)
        n_send = 9 + n_dp // n_mp
        n_recv = 3 * (n_mp - 1) + 8 + n_dp // 2 + PARTS * n_dp
        vmem = pl.BlockSpec(memory_space=pltpu.VMEM)
        shapes = (
            jax.ShapeDtypeStruct((ql, cols), BF),
            jax.ShapeDtypeStruct((ql, cols), BF),
            jax.ShapeDtypeStruct((chunk, cols), F32),
        )
        found = pl.pallas_call(
            functools.partial(kernel, n_dp, n_mp),
            out_shape=shapes,
            in_specs=[pl.BlockSpec(memory_space=pltpu.HBM)] * 7,
            out_specs=(vmem, vmem, vmem),
            scratch_shapes=[
                pltpu.VMEM((ql, cols), BF),
                pltpu.VMEM((ql, cols), BF),
                pltpu.SMEM(logit_scale.shape, F32),
                pltpu.VMEM(loss_grad.shape[::-1], F32),
                pltpu.VMEM(shortlist.shape, jnp.int32),
                pltpu.VMEM(send_rows.shape, jnp.int32),
                pltpu.VMEM((total, cols), BF),
                pltpu.VMEM((n_mp, 2, ql, cols), BF),
                pltpu.VMEM((cols, 2 * ql), BF),
                pltpu.VMEM((2, n_dp // 2, chunk, 2 * ql), BF),
                pltpu.VMEM((n_dp, blk, cols), BF),
                pltpu.VMEM((n_dp, blk, cols), BF),
                pltpu.VMEM((ql + 8, slots), F32),
                pltpu.VMEM((n_mp, ql + 8, slots), F32),
                pltpu.VMEM((n_loc * ql, slots), BF),
                pltpu.VMEM((n_dp, blk, cols), BF),
                pltpu.VMEM((n_dp, blk, cols), BF),
                pltpu.VMEM((n_dp, 2, ql, cols), BF),
                pltpu.VMEM((2, n_mp - 1, ql, cols), BF),
                pltpu.VMEM((2, n_mp - 1, ql, cols), BF),
                pltpu.VMEM((slots, cols), F32),
                pltpu.SemaphoreType.DMA((n_send,)),
                pltpu.SemaphoreType.DMA((n_recv,)),
                pltpu.SemaphoreType.DMA((8,)),
            ],
            compiler_params=pltpu.CompilerParams(
                collective_id=0, has_side_effects=True, vmem_limit_bytes=48 << 20
            ),
        )(
            *[
                pltpu.with_memory_space_constraint(x, pltpu.HBM)
                for x in (
                    query_rows,
                    doc_rows,
                    head,
                    logit_scale,
                    loss_grad.T,
                    shortlist,
                    send_rows,
                )
            ]
        )
        return pl.pallas_call(
            hand_on,
            out_shape=shapes,
            in_specs=[vmem] * 3,
            out_specs=(pl.BlockSpec(memory_space=pltpu.HBM),) * 3,
            scratch_shapes=[pltpu.SemaphoreType.DMA((3,))],
            compiler_params=pltpu.CompilerParams(vmem_limit_bytes=8 << 20),
        )(*found)

    return jax.shard_map(
        on_device,
        mesh=mesh,
        in_specs=(
            P("dp", "mp"),
            P("dp", "mp"),
            P(None, "mp"),
            P(),
            P("dp", None),
            P("dp", None),
            P("dp", None),
        ),
        out_specs=(P("dp", "mp"), P("dp", "mp"), P("dp", "mp")),
        check_vma=False,
    )
```
